128 devices in a mesh: seq: 64 (over x, z, y), head: 2 (over core).
Axes of the slice: x: 4, y: 4, z: 4, core: 2. Of those that a mesh axis runs over, the one named last changes fastest.
Arguments:
- queries: bfloat16 [16384, 4096], P('seq', 'head'), may hold values from -210 to 210
- keys: bfloat16 [16384, 1024], P('seq', 'head'), may hold values from -7 to 7
- values: bfloat16 [16384, 1024], P('seq', 'head'), may hold values from -6 to 6
- vertical: int32 [8, 64], P('head'), may hold values from 0 to 255, as said below
- slash: int32 [8, 2], P('head'), may hold values from 1 to 4, as said below
- out_weight: bfloat16 [4096, 4096], P('head'), may hold values from -1 to 1
Outputs:
- mixed: bfloat16 [16384, 4096], P(('seq', 'head'))
The draws below stay inside these ranges and needn't reach their ends.
Inputs may be any that keep to these rules, and one draw needn't show every extreme that they name: `vertical`: for each key-value head, 64 different key blocks in increasing order; block b lies in slab b // 4; no slab holds more than 2 of one head's blocks, and for every head some slab holds exactly 2. `slash`: for each key-value head, 2 different offsets in increasing order; some head has the offset 256 // 64.
All inputs are finite; a program needn't handle non-finite values.
Results may differ from the reference program's by a relative error of at most 0.01.
Values may be sent and summed in bfloat16 or wider, within the bound.
A program may use at most 128 MiB of HBM per device.

```python
from functools import partial
import jax
import jax.numpy as jnp
from jax import lax

HEADS = 32
KEY_VALUE_HEADS = 8
HEAD_DIM = 128
DMODEL = 4096
S_DEV = 256
BLK = 64
NS = 2
CAP = 2
NV = 64
SEQ = 16384
N_SEQ = 64


def paired(key):
    key_seed, query_seed = jax.random.split(jax.random.fold_in(key, 7), 2)
    keys_f = jnp.clip(jax.random.normal(key_seed, (SEQ, KEY_VALUE_HEADS * HEAD_DIM), jnp.float32), -6.0, 6.0)
    query_f = jnp.clip(1.5 * jax.random.normal(query_seed, (SEQ, HEADS * HEAD_DIM), jnp.float32), -9.0, 9.0)
    return (query_f, keys_f)


def draw_queries(key, part):
    return paired(key)[0].astype(jnp.bfloat16)


def draw_keys(key, part):
    return paired(key)[1].astype(jnp.bfloat16)


def draw_vertical(key, part):
    block_span = S_DEV // BLK
    owners = SEQ // S_DEV
    perm_seed, score_seed, force_seed = jax.random.split(jax.random.fold_in(key, 3), 3)
    within = jax.random.randint(perm_seed, (KEY_VALUE_HEADS, owners, block_span), 0, 1 << 20) * block_span + jnp.arange(block_span, dtype=jnp.int32)
    order = jnp.argsort(within, axis=-1)[:, :, :CAP]
    blocks = (order + jnp.arange(owners, dtype=jnp.int32)[None, :, None] * block_span).reshape(KEY_VALUE_HEADS, owners * CAP)
    owner_of = jnp.repeat(jnp.arange(owners, dtype=jnp.int32), CAP)
    forced_blocks = jax.random.randint(force_seed, (KEY_VALUE_HEADS, 1), 0, owners)
    block_score = jax.random.randint(score_seed, (KEY_VALUE_HEADS, owners * CAP), 0, 4096) + (owners - owner_of)[None, :] * (8192 // owners)
    block_score = block_score + jnp.where(owner_of[None, :] == forced_blocks, 1 << 16, 0)
    block_score = block_score * (owners * CAP) + jnp.arange(owners * CAP, dtype=jnp.int32)[None, :]
    unused, picked = lax.top_k(block_score, NV)
    chosen = jnp.take_along_axis(blocks, picked, axis=1)
    return jnp.sort(chosen, axis=1).astype(jnp.int32)


def draw_slash(key, part):
    block_span = S_DEV // BLK
    score_seed, force_seed = jax.random.split(jax.random.fold_in(key, 5), 2)
    block_score = jax.random.randint(score_seed, (KEY_VALUE_HEADS, block_span), 0, 4096) * block_span + jnp.arange(block_span, dtype=jnp.int32)[None, :]
    forced_blocks = jax.random.randint(force_seed, (), 0, KEY_VALUE_HEADS)
    extra_score = (jnp.arange(KEY_VALUE_HEADS)[:, None] == forced_blocks) & (jnp.arange(block_span)[None, :] == block_span - 1)
    block_score = block_score + jnp.where(extra_score, 1 << 24, 0)
    unused, picked = lax.top_k(block_score, NS)
    return jnp.sort(picked + 1, axis=1).astype(jnp.int32)


def block_scale(key, shape, pieces, least, top_value):
    def one(position, blocks):
        steps = jax.random.uniform(jax.random.fold_in(jax.random.fold_in(key, 6), position), (blocks,), jnp.float32, least / len(pieces), top_value / len(pieces))
        return jnp.repeat(jnp.exp(steps), shape[position] // blocks).reshape((-1,) + (1,) * (len(shape) - position - 1))

    loudness = one(*pieces[0])
    for cut in pieces[1:]:
        loudness = loudness * one(*cut)
    return loudness


def bell_draw(key, shape, scale, bound, pieces=(), held_as=jnp.bfloat16):
    factor_of = block_scale(key, shape, pieces, -0.22, 0.18) if pieces else 1.0
    array = jax.random.normal(key, shape, jnp.float32) * scale * factor_of
    return jnp.minimum(jnp.maximum(array, -bound), bound).astype(held_as)


def setup_inputs(seed: int = 0) -> dict:
    splits = jax.random.split(jax.random.key(seed), 7)
    return {
        "queries": draw_queries(jax.random.fold_in(splits[6], 71), 0),
        "keys": draw_keys(jax.random.fold_in(splits[6], 71), 0),
        "values": bell_draw(splits[2], (SEQ, KEY_VALUE_HEADS * HEAD_DIM), 1.0, 6.0, ((0, 64), (1, 2))),
        "vertical": draw_vertical(jax.random.fold_in(splits[6], 71), 0),
        "slash": draw_slash(jax.random.fold_in(splits[6], 71), 0),
        "out_weight": bell_draw(splits[5], (HEADS * HEAD_DIM, DMODEL), HEADS ** -0.5, 1.0, ((0, 2),)),
    }


NEGATIVE = -1e30


def attended_block_tile(block_index, vert_ids, slash_ids, key_head, value_head, query_head_index, causal):
    offsets = jnp.concatenate([jnp.zeros((1,), jnp.int32), slash_ids.astype(jnp.int32)])
    diagonal = block_index - offsets
    vert_ok = (vert_ids < block_index) & jnp.all(block_index - vert_ids[:, None] != slash_ids[None, :], axis=1)
    diag_ok = diagonal >= 0
    chosen = jnp.concatenate([vert_ids.astype(jnp.int32), jnp.maximum(diagonal, 0).astype(jnp.int32)])
    usable = jnp.concatenate([vert_ok, diag_ok])
    gathered_keys = key_head[chosen].reshape(-1, HEAD_DIM)
    gathered_values = value_head[chosen].reshape(-1, HEAD_DIM)
    same_block = chosen == block_index
    allowed = usable[None, :, None] & (jnp.logical_not(same_block)[None, :, None] | causal[:, None, :])
    allowed = allowed.reshape(BLK, -1)
    query_block_tile = query_head_index[block_index]
    scores = jnp.einsum("qgd,kd->gqk", query_block_tile.astype(jnp.float32), gathered_keys.astype(jnp.float32)) * (HEAD_DIM ** -0.5)
    scores = jnp.where(allowed[None], scores, NEGATIVE)
    top_score = jnp.max(scores, axis=-1, keepdims=True)
    weights = jnp.where(allowed[None], jnp.exp(scores - top_score), 0.0)
    sum_weight = jnp.sum(weights, axis=-1, keepdims=True)
    rounded = lax.optimization_barrier(weights.astype(jnp.bfloat16)).astype(jnp.float32)
    output = jnp.einsum("gqk,kd->gqd", rounded, gathered_values.astype(jnp.float32)) / sum_weight
    return output.transpose(1, 0, 2).astype(jnp.bfloat16)


def attend_slab(slab_start, block_fn, slab_blocks):
    return jax.vmap(block_fn)(slab_start + jnp.arange(slab_blocks, dtype=jnp.int32))


def reference(queries, keys, values, vertical, slash, out_weight):
    per_group = HEADS // KEY_VALUE_HEADS
    block_count = SEQ // BLK
    slab_blocks = S_DEV // BLK
    query_blocks = queries.reshape(block_count, BLK, KEY_VALUE_HEADS, per_group, HEAD_DIM)
    key_blocks = keys.reshape(block_count, BLK, KEY_VALUE_HEADS, HEAD_DIM)
    value_blocks = values.reshape(block_count, BLK, KEY_VALUE_HEADS, HEAD_DIM)
    within = jnp.arange(BLK)
    causal = within[None, :] <= within[:, None]
    results = []
    for head_index in range(KEY_VALUE_HEADS):
        block_fn = partial(attended_block_tile, vert_ids=vertical[head_index], slash_ids=slash[head_index],
                           key_head=key_blocks[:, :, head_index], value_head=value_blocks[:, :, head_index],
                           query_head_index=query_blocks[:, :, head_index], causal=causal)
        mapped = lax.map(partial(attend_slab, block_fn=block_fn, slab_blocks=slab_blocks),
                         jnp.arange(N_SEQ, dtype=jnp.int32) * slab_blocks)
        results.append(mapped.reshape(SEQ, per_group * HEAD_DIM))
    attention = jnp.concatenate(results, axis=1)
    return jnp.dot(attention, out_weight, preferred_element_type=jnp.float32).astype(jnp.bfloat16)
```

```python
import functools
import math

import jax
import jax.numpy as jnp
from jax import lax
from jax.experimental import pallas as pl
from jax.experimental.pallas import tpu as pltpu
from jax.sharding import PartitionSpec as P

HEAD_DIM = 128
BLK = 64
CAP = 2
NEGATIVE = -1e30
MESH = pl.DeviceIdType.MESH
SCALE = HEAD_DIM ** (-0.5) * math.log2(math.e)
SIDE = 4
FAR_CHUNK = 8


def kernel(
    per_group, tile,
    q_ref, k_ref, v_ref, vert_ref, slash_ref, w_hbm, out_ref,
    pack, slots, qg, kg, vg, kc, vtc, w_ref, acc, top, total, o_buf, attn, res, give, take,
    w_sem, pack_send, kv_send, kv_recv, q_send, q_recv, slot_recv, ring_send,
    o_send, o_recv, x_send, x_recv,
):
    rows = q_ref.shape[0]
    me = lax.axis_index("seq")
    core = lax.axis_index("head")
    other = 1 - core
    o, c = me // SIDE, me % SIDE
    x, z = o // SIDE, o % SIDE
    slab_blocks = rows // BLK
    half = rows // 2
    width = per_group * HEAD_DIM
    chosen_count = vert_ref.shape[1]
    next_plane = (me + SIDE) % (SIDE ** 3)
    last_plane = (me + SIDE ** 3 - SIDE) % (SIDE ** 3)

    def at(xx, zz, cc):
        return (xx % SIDE * SIDE + zz % SIDE) * SIDE + cc

    barrier = pltpu.get_barrier_semaphore()

    def greet(seq, head):
        pl.semaphore_signal(barrier, inc=1, device_id=(seq, head), device_id_type=MESH)

    greet(me, other)
    for d in range(1, SIDE):
        greet(o * SIDE + (c + d) % SIDE, core)
    for step in (1, SIDE - 1):
        greet(at(x + step, z, c), core)
        greet(at(x, z + step, c), core)
    greet(next_plane, core)
    greet(last_plane, core)

    weight_copy = pltpu.make_async_copy(w_hbm, w_ref, w_sem)
    weight_copy.start()

    def lanes(h, size=HEAD_DIM):
        return pl.ds(pl.multiple_of(h * size, size), size)

    first_block = me * slab_blocks
    for h in range(SIDE):
        low, high = jnp.int32(slab_blocks), jnp.int32(-1)
        for e in range(chosen_count):
            block = vert_ref[h, e] - first_block
            inside = (block >= 0) & (block < slab_blocks)
            low = jnp.where(inside, jnp.minimum(low, block), low)
            high = jnp.where(inside, jnp.maximum(high, block), high)
        for slot, block in enumerate((low, high)):
            for part, source in enumerate((k_ref, v_ref)):
                got = source[:BLK, h * HEAD_DIM:(h + 1) * HEAD_DIM]
                for i in range(1, slab_blocks):
                    rows_i = source[i * BLK:(i + 1) * BLK, h * HEAD_DIM:(h + 1) * HEAD_DIM]
                    got = jnp.where(block == i, rows_i, got)
                pack[h, part * CAP + slot] = got
    for i in range(2 * CAP):
        slots[me * (2 * CAP) + i] = pack[c, i]
    kg[c + 1] = k_ref[:, lanes(c)]
    vg[c + 1] = v_ref[:, lanes(c)]
    qg[c] = q_ref[:, lanes(c, width)]

    pl.semaphore_wait(barrier, 1 + (SIDE - 1) + 4 + 2)

    def remote(src, dst, send_sem, recv_sem, seq):
        return pltpu.make_async_remote_copy(
            src_ref=src, dst_ref=dst, send_sem=send_sem, recv_sem=recv_sem,
            device_id=(seq, core), device_id_type=MESH,
        )

    def held(slab):
        return slots.at[pl.ds(slab * (2 * CAP), 2 * CAP)]

    def peer(d):
        return (c + d) % SIDE

    def pack_copy(d):
        return remote(pack.at[peer(d)], held(me), pack_send.at[d], slot_recv.at[me], o * SIDE + peer(d))

    def kv_copies(d):
        to = peer(d)
        return [
            remote(source.at[:, lanes(to)], got.at[c + 1], kv_send.at[d, i], kv_recv.at[c + 1, i], o * SIDE + to)
            for i, (source, got) in enumerate(((k_ref, kg), (v_ref, vg)))
        ]

    def q_copy(d):
        to = peer(d)
        return remote(q_ref.at[:, lanes(to, width)], qg.at[c], q_send.at[d], q_recv.at[c], o * SIDE + to)

    def next_copies():
        return [
            remote(got.at[SIDE], got.at[0], kv_send.at[0, i], kv_recv.at[0, i], next_plane)
            for i, got in enumerate((kg, vg))
        ]

    near_order = (1, SIDE - 1, 2)
    for d in near_order:
        pack_copy(d).start()
    for d in near_order:
        for copy in kv_copies(d):
            copy.start()
    for d in near_order:
        q_copy(d).start()

    def slab_of(dp, dq, kind):
        dx, dz = (dp, dq) if kind < 2 else (dq, dp)
        return at(x + SIDE - dx, z + SIDE - dz, kind)

    def ring(slab, kind, phase, sign):
        along_x = (kind < 2) == (phase == 0)
        to = at(x + SIDE + sign, z, c) if along_x else at(x, z + SIDE + sign, c)
        there = held(slab)
        way = (0 if along_x else 2) + (sign > 0)
        return remote(there, there, ring_send.at[slab, way], slot_recv.at[slab], to)

    def arrived(slab):
        there = held(slab)
        remote(there, there, ring_send.at[slab, 0], slot_recv.at[slab], next_plane).wait_recv()

    def sign_of(kind):
        return 1 if kind % 2 == 0 else -1

    def own(act):
        for kind in range(SIDE):
            slab = slab_of(0, 0, kind)
            act(slab, kind, [(0, 1), (0, -1), (1, 1), (1, -1)])

    def first(dp, act):
        for kind in range(SIDE):
            ways = [(0, dp)] if dp == sign_of(kind) else []
            act(slab_of(dp, 0, kind), kind, ways + [(1, 1), (1, -1)])

    def second(dp, dq, act):
        for kind in range(SIDE):
            act(slab_of(dp, dq, kind), kind, [(1, dq)] if dq == sign_of(kind) else [])

    def pass_on(slab, kind, ways):
        arrived(slab)
        for phase, sign in ways:
            ring(slab, kind, phase, sign).start()

    def pass_own(slab, kind, ways):
        @pl.when(c != kind)
        def _():
            arrived(slab)

        for phase, sign in ways:
            ring(slab, kind, phase, sign).start()

    def sent(slab, kind, ways):
        for phase, sign in ways:
            ring(slab, kind, phase, sign).wait_send()

    own(pass_own)
    for dp in (1, -1, 2):
        first(dp, pass_on)

    for d in range(1, SIDE):
        for i, got in enumerate((kg, vg)):
            there = got.at[peer(d) + 1]
            remote(there, there, kv_send.at[d, i], kv_recv.at[peer(d) + 1, i], next_plane).wait_recv()
    for copy in next_copies():
        copy.start()
    for copy in next_copies():
        copy.wait_recv()

    heads = range(per_group)

    def near(i):
        base = (o * SIDE + i) * slab_blocks
        k = jnp.concatenate([kg[i], kg[i + 1]], axis=0)
        vt = jnp.concatenate([vg[i], vg[i + 1]], axis=0).T
        shape = (2 * slab_blocks, rows)
        block = lax.broadcasted_iota(jnp.int32, shape, 0) - slab_blocks
        gap = lax.broadcasted_iota(jnp.int32, shape, 1) // BLK - block
        block = base + block
        good = gap == 0
        for j in range(slash_ref.shape[1]):
            good = good | (gap == slash_ref[c, j])
        chosen = block == vert_ref[c, 0]
        for e in range(1, chosen_count):
            chosen = chosen | (block == vert_ref[c, e])
        good = good | (chosen & (gap > 0))
        bias = jnp.where(good & (block >= 0), 0.0, NEGATIVE)
        keys_at = lax.broadcasted_iota(jnp.int32, (rows, rows), 0)
        query_at = lax.broadcasted_iota(jnp.int32, (rows, rows), 1)
        causal = keys_at <= query_at
        scores = []
        for g in heads:
            q = qg[i, :, g * HEAD_DIM:(g + 1) * HEAD_DIM]
            scores.append(lax.dot_general(k, q, (((1,), (1,)), ((), ())), preferred_element_type=jnp.float32))
        for g, s in zip(heads, scores):
            s = s * SCALE
            s = jnp.concatenate(
                [s[j * BLK:(j + 1) * BLK] + bias[j:j + 1] for j in range(2 * slab_blocks)], axis=0)
            s = jnp.concatenate([s[:rows], jnp.where(causal, s[rows:], NEGATIVE)], axis=0)
            peak = jnp.max(s, axis=0, keepdims=True)
            p = jnp.exp2(s - peak)
            top[i, g] = peak
            total[i, g] = jnp.sum(p, axis=0, keepdims=True)
            acc[i, g] = jnp.dot(vt, p.astype(jnp.bfloat16), preferred_element_type=jnp.float32)

    def near_and_pass(step, _):
        i = (c + step) % SIDE

        @pl.when(step > 0)
        def _():
            remote(qg.at[i], qg.at[i], q_send.at[1], q_recv.at[i], next_plane).wait_recv()

        for dq in (1, -1):
            second(step, dq, pass_on)
        near(i)
        return 0

    lax.fori_loop(0, SIDE, near_and_pass, 0)

    def last_ones(step, _):
        second(step, 2, lambda slab, kind, ways: arrived(slab))
        return 0

    lax.fori_loop(0, SIDE, last_ones, 0)

    limit = (o * SIDE + lax.broadcasted_iota(jnp.int32, (BLK, HEAD_DIM), 1) - 1) * slab_blocks
    chunks = jnp.minimum(chosen_count // FAR_CHUNK, o + 1)

    def collect(pair, _):
        got = []
        for j in range(2):
            e = pair * 2 + j
            slab = vert_ref[c, e] // slab_blocks
            before = jnp.where(e > 0, vert_ref[c, jnp.maximum(e - 1, 0)] // slab_blocks, -1)
            place = slab * (2 * CAP) + jnp.where(before == slab, 1, 0)
            at_row = pl.ds(pl.multiple_of(e * BLK, BLK), BLK)
            kc[at_row, :HEAD_DIM] = slots[place]
            kc[at_row, HEAD_DIM:] = jnp.where(vert_ref[c, e] < limit, 0.0, NEGATIVE).astype(jnp.bfloat16)
            got.append(slots[place + CAP])
        vtc[pair] = jnp.concatenate(got, axis=0).T
        return 0

    lax.fori_loop(0, chunks * (FAR_CHUNK // 2), collect, 0)

    def o_copy(i, to):
        return remote(o_buf.at[i], attn.at[c], o_send.at[i], o_recv.at[c], o * SIDE + to)

    def far_slab(step, _):
        i = (c + SIDE - 1 - step) % SIDE
        mark = (lax.broadcasted_iota(jnp.int32, (rows, HEAD_DIM), 1) == i).astype(jnp.bfloat16)

        def chunk(n, _):
            k = kc[pl.ds(pl.multiple_of(n * FAR_CHUNK * BLK, FAR_CHUNK * BLK), FAR_CHUNK * BLK), :]
            vt = jnp.concatenate([vtc[n * (FAR_CHUNK // 2) + j] for j in range(FAR_CHUNK // 2)], axis=1)
            scores = []
            old = [(top[i, g], total[i, g]) for g in heads]
            for g in heads:
                q = jnp.concatenate([qg[i, :, g * HEAD_DIM:(g + 1) * HEAD_DIM], mark], axis=1)
                scores.append(lax.dot_general(k, q, (((1,), (1,)), ((), ())), preferred_element_type=jnp.float32))
            done = []
            for s, (peak_old, amount_old) in zip(scores, old):
                s = s * SCALE
                peak = jnp.maximum(peak_old, jnp.max(s, axis=0, keepdims=True))
                shrink = jnp.exp2(peak_old - peak)
                p = jnp.exp2(s - peak)
                amount = amount_old * shrink + jnp.sum(p, axis=0, keepdims=True)
                mix = jnp.dot(vt, p.astype(jnp.bfloat16), preferred_element_type=jnp.float32)
                done.append((peak, amount, shrink, mix))
            for g, (peak, amount, shrink, mix) in zip(heads, done):
                top[i, g] = peak
                total[i, g] = amount
                acc[i, g] = acc[i, g] * shrink + mix
            return 0

        lax.fori_loop(0, chunks, chunk, 0)
        for g in heads:
            a = acc[i, g] * (1.0 / total[i, g])
            o_buf[i, :, g * HEAD_DIM:(g + 1) * HEAD_DIM] = a.T.astype(jnp.bfloat16)

        @pl.when(step < SIDE - 1)
        def _():
            o_copy(i, i).start()

        return 0

    lax.fori_loop(0, SIDE, far_slab, 0)
    attn[c] = o_buf[c]
    for d in range(1, SIDE):
        there = attn.at[peer(d)]
        remote(there, there, o_send.at[peer(d)], o_recv.at[peer(d)], next_plane).wait_recv()

    weight_copy.wait()
    tiles = give.shape[0]
    mine = pl.ds(pl.multiple_of(core * half, half), half)
    theirs = pl.ds(pl.multiple_of(other * half, half), half)

    def swap(t):
        return pltpu.make_async_remote_copy(
            src_ref=give.at[t], dst_ref=take.at[t], send_sem=x_send.at[t], recv_sem=x_recv.at[t],
            device_id=(me, other), device_id_type=MESH,
        )

    def project(t, _):
        columns = pl.ds(pl.multiple_of(t * tile, tile), tile)
        a = jnp.concatenate([attn[j] for j in range(SIDE)], axis=1)
        res[t] = jnp.dot(a, w_ref[:, columns], preferred_element_type=jnp.float32)
        give[t] = res[t, theirs, :].astype(jnp.bfloat16)
        swap(t).start()
        return 0

    lax.fori_loop(0, tiles, project, 0)

    def add_up(t, _):
        columns = pl.ds(pl.multiple_of(t * tile, tile), tile)
        swap(t).wait_recv()
        out_ref[:, columns] = (res[t, mine, :] + take[t].astype(jnp.float32)).astype(out_ref.dtype)
        return 0

    lax.fori_loop(0, tiles, add_up, 0)

    def swapped(t, _):
        swap(t).wait_send()
        return 0

    lax.fori_loop(0, tiles, swapped, 0)
    for d in range(1, SIDE):
        pack_copy(d).wait_send()
        for copy in kv_copies(d):
            copy.wait_send()
        q_copy(d).wait_send()
        o_copy(peer(d), peer(d)).wait_send()
    for copy in next_copies():
        copy.wait_send()
    own(sent)
    for dp in (1, -1, 2):
        first(dp, sent)

    def ring_sent(step, _):
        for dq in (1, -1):
            second(step, dq, sent)
        return 0

    lax.fori_loop(0, SIDE, ring_sent, 0)


def on_device(n, queries, keys, values, vertical, slash, out_weight):
    rows = queries.shape[0]
    kv = vertical.shape[0]
    per_group = queries.shape[1] // (kv * HEAD_DIM)
    width = per_group * HEAD_DIM
    model = out_weight.shape[1]
    listed = vertical.shape[1]

    tile = math.gcd(model, 512)
    tiles = model // tile
    vmem = pl.BlockSpec(memory_space=pltpu.VMEM)
    smem = pl.BlockSpec(memory_space=pltpu.SMEM)
    dma = pltpu.SemaphoreType.DMA
    return pl.pallas_call(
        functools.partial(kernel, per_group, tile),
        out_shape=jax.ShapeDtypeStruct((rows // 2, model), jnp.bfloat16),
        in_specs=[vmem] * 3 + [smem] * 2 + [pl.BlockSpec(memory_space=pl.ANY)],
        out_specs=vmem,
        scratch_shapes=[
            pltpu.VMEM((kv, 2 * CAP, BLK, HEAD_DIM), jnp.bfloat16),
            pltpu.VMEM((n * 2 * CAP, BLK, HEAD_DIM), jnp.bfloat16),
            pltpu.VMEM((SIDE, rows, width), jnp.bfloat16),
            pltpu.VMEM((SIDE + 1, rows, HEAD_DIM), jnp.bfloat16),
            pltpu.VMEM((SIDE + 1, rows, HEAD_DIM), jnp.bfloat16),
            pltpu.VMEM((listed * BLK, 2 * HEAD_DIM), jnp.bfloat16),
            pltpu.VMEM((listed // 2, HEAD_DIM, 2 * BLK), jnp.bfloat16),
            pltpu.VMEM(out_weight.shape, jnp.bfloat16),
            pltpu.VMEM((SIDE, per_group, HEAD_DIM, rows), jnp.float32),
            pltpu.VMEM((SIDE, per_group, 1, rows), jnp.float32),
            pltpu.VMEM((SIDE, per_group, 1, rows), jnp.float32),
            pltpu.VMEM((SIDE, rows, width), jnp.bfloat16),
            pltpu.VMEM((SIDE, rows, width), jnp.bfloat16),
            pltpu.VMEM((tiles, rows, tile), jnp.float32),
            pltpu.VMEM((tiles, rows // 2, tile), jnp.bfloat16),
            pltpu.VMEM((tiles, rows // 2, tile), jnp.bfloat16),
            dma,
            dma((SIDE,)),
            dma((SIDE, 2)),
            dma((SIDE + 1, 2)),
            dma((SIDE,)),
            dma((SIDE,)),
            dma((n,)),
            dma((n, SIDE)),
            dma((SIDE,)),
            dma((SIDE,)),
            dma((tiles,)),
            dma((tiles,)),
        ],
        compiler_params=pltpu.CompilerParams(
            collective_id=0, has_side_effects=True, vmem_limit_bytes=60 * 2**20
        ),
    )(queries, keys, values, vertical, slash, out_weight)


def solution(mesh):
    placed = (
        P("seq", "head"),
        P("seq", "head"),
        P("seq", "head"),
        P("head", None),
        P("head", None),
        P("head", None),
    )
    return jax.shard_map(
        functools.partial(on_device, mesh.shape["seq"]),
        mesh=mesh, in_specs=placed, out_specs=P(("seq", "head"), None), check_vma=False,
    )
```

```python
import functools
import math

import jax
import jax.numpy as jnp
from jax import lax
from jax.experimental import pallas as pl
from jax.experimental.pallas import tpu as pltpu
from jax.sharding import PartitionSpec as P

HEAD_DIM = 128
BLK = 64
CAP = 2
NEGATIVE = -1e30
MESH = pl.DeviceIdType.MESH
SCALE = HEAD_DIM ** (-0.5) * math.log2(math.e)
SIDE = 4
FAR_CHUNK = 16
AUX = 16


def kernel(
    per_group, tile,
    q_ref, k_ref, v_ref, vert_ref, slash_ref, w_hbm, out_ref,
    packs, slots, qg, qt, kg, vg, kc, vtc, w_ref, acc, top, total, o_buf, attn, res, give, take,
    w_sem, pack_send, kv_send, kv_recv, q_send, q_recv, slot_recv, ring_send,
    o_send, o_recv, x_send, x_recv,
):
    rows = q_ref.shape[0]
    me = lax.axis_index("seq")
    core = lax.axis_index("head")
    other = 1 - core
    o, c = me // SIDE, me % SIDE
    x, z = o // SIDE, o % SIDE
    slab_blocks = rows // BLK
    half = rows // 2
    width = per_group * HEAD_DIM
    chosen_count = vert_ref.shape[1]
    next_plane = (me + SIDE) % (SIDE ** 3)
    last_plane = (me + SIDE ** 3 - SIDE) % (SIDE ** 3)

    def at(xx, zz, cc):
        return (xx % SIDE * SIDE + zz % SIDE) * SIDE + cc

    barrier = pltpu.get_barrier_semaphore()

    def greet(seq, head):
        pl.semaphore_signal(barrier, inc=1, device_id=(seq, head), device_id_type=MESH)

    greet(me, other)
    for d in range(1, SIDE):
        greet(o * SIDE + (c + d) % SIDE, core)
    for step in (1, SIDE - 1):
        greet(at(x + step, z, c), core)
        greet(at(x, z + step, c), core)
    greet(next_plane, core)
    greet(last_plane, core)

    weight_copy = pltpu.make_async_copy(w_hbm, w_ref, w_sem)
    weight_copy.start()

    def lanes(h, size=HEAD_DIM):
        return pl.ds(pl.multiple_of(h * size, size), size)

    first_block = me * slab_blocks
    for h in range(SIDE):
        low, high = jnp.int32(slab_blocks), jnp.int32(-1)
        for e in range(chosen_count):
            block = vert_ref[h, e] - first_block
            inside = (block >= 0) & (block < slab_blocks)
            low = jnp.where(inside, jnp.minimum(low, block), low)
            high = jnp.where(inside, jnp.maximum(high, block), high)
        for slot, block in enumerate((low, high)):
            for part, source in enumerate((k_ref, v_ref)):
                got = source[:BLK, h * HEAD_DIM:(h + 1) * HEAD_DIM]
                for i in range(1, slab_blocks):
                    rows_i = source[i * BLK:(i + 1) * BLK, h * HEAD_DIM:(h + 1) * HEAD_DIM]
                    got = jnp.where(block == i, rows_i, got)
                packs[part][h, slot] = got
    for part in range(2):
        for i in range(CAP):
            slots[part][me * CAP + i] = packs[part][c, i]
    kg[c + 1] = k_ref[:, lanes(c)]
    vg[c + 1] = v_ref[:, lanes(c)]
    qg[c] = q_ref[:, lanes(c, width)]

    pl.semaphore_wait(barrier, 1 + (SIDE - 1) + 4 + 2)

    def remote(src, dst, send_sem, recv_sem, seq):
        return pltpu.make_async_remote_copy(
            src_ref=src, dst_ref=dst, send_sem=send_sem, recv_sem=recv_sem,
            device_id=(seq, core), device_id_type=MESH,
        )

    def held(part, slab):
        return slots[part].at[pl.ds(slab * CAP, CAP)]

    def peer(d):
        return (c + d) % SIDE

    def pack_copy(part, d):
        return remote(packs[part].at[peer(d)], held(part, me), pack_send.at[part, d], slot_recv.at[part, me],
                      o * SIDE + peer(d))

    def kv_copies(d):
        to = peer(d)
        return [
            remote(source.at[:, lanes(to)], got.at[c + 1], kv_send.at[d, i], kv_recv.at[c + 1, i], o * SIDE + to)
            for i, (source, got) in enumerate(((k_ref, kg), (v_ref, vg)))
        ]

    def q_copy(d):
        to = peer(d)
        return remote(q_ref.at[:, lanes(to, width)], qg.at[c], q_send.at[d], q_recv.at[c], o * SIDE + to)

    def next_copies():
        return [
            remote(got.at[SIDE], got.at[0], kv_send.at[0, i], kv_recv.at[0, i], next_plane)
            for i, got in enumerate((kg, vg))
        ]

    near_order = (1, SIDE - 1, 2)
    for part in range(2):
        for d in near_order:
            pack_copy(part, d).start()
    for d in near_order:
        for copy in kv_copies(d):
            copy.start()
    for d in near_order:
        q_copy(d).start()

    def slab_of(dp, dq, kind):
        dx, dz = (dp, dq) if kind < 2 else (dq, dp)
        return at(x + SIDE - dx, z + SIDE - dz, kind)

    def ring(part, slab, kind, phase, sign):
        along_x = (kind < 2) == (phase == 0)
        to = at(x + SIDE + sign, z, c) if along_x else at(x, z + SIDE + sign, c)
        there = held(part, slab)
        way = (0 if along_x else 2) + (sign > 0)
        return remote(there, there, ring_send.at[part, slab, way], slot_recv.at[part, slab], to)

    def arrived(part, slab):
        there = held(part, slab)
        remote(there, there, pack_send.at[part, 1], slot_recv.at[part, slab], next_plane).wait_recv()

    def sign_of(kind):
        return 1 if kind % 2 == 0 else -1

    def own(act):
        for kind in range(SIDE):
            slab = slab_of(0, 0, kind)
            act(slab, kind, [(0, 1), (0, -1), (1, 1), (1, -1)])

    def first(dp, act):
        for kind in range(SIDE):
            ways = [(0, dp)] if dp == sign_of(kind) else []
            act(slab_of(dp, 0, kind), kind, ways + [(1, 1), (1, -1)])

    def second(dp, dq, act):
        for kind in range(SIDE):
            act(slab_of(dp, dq, kind), kind, [(1, dq)] if dq == sign_of(kind) else [])

    def pass_on(part):
        def act(slab, kind, ways):
            arrived(part, slab)
            for phase, sign in ways:
                ring(part, slab, kind, phase, sign).start()

        return act

    def pass_own(part):
        def act(slab, kind, ways):
            @pl.when(c != kind)
            def _():
                arrived(part, slab)

            for phase, sign in ways:
                ring(part, slab, kind, phase, sign).start()

        return act

    def sent(part):
        def act(slab, kind, ways):
            for phase, sign in ways:
                ring(part, slab, kind, phase, sign).wait_send()

        return act

    own(pass_own(0))
    for dp in (1, -1, 2):
        first(dp, pass_on(0))
    own(pass_own(1))

    for d in range(1, SIDE):
        for i, got in enumerate((kg, vg)):
            there = got.at[peer(d) + 1]
            remote(there, there, kv_send.at[d, i], kv_recv.at[peer(d) + 1, i], next_plane).wait_recv()
    for copy in next_copies():
        copy.start()

    heads = range(per_group)

    def turn(i):
        row = lax.broadcasted_iota(jnp.int32, (HEAD_DIM, rows), 0)
        for g in heads:
            qt[i, g, :HEAD_DIM] = qg[i, :, g * HEAD_DIM:(g + 1) * HEAD_DIM].T
            qt[i, g, HEAD_DIM:] = jnp.where(row == i, 1.0, 0.0).astype(jnp.bfloat16)

    def near(i):
        base = (o * SIDE + i) * slab_blocks
        k = jnp.concatenate([kg[i], kg[i + 1]], axis=0)
        vt = jnp.concatenate([vg[i], vg[i + 1]], axis=0).T
        shape = (2 * slab_blocks, rows)
        block = lax.broadcasted_iota(jnp.int32, shape, 0) - slab_blocks
        gap = lax.broadcasted_iota(jnp.int32, shape, 1) // BLK - block
        block = base + block
        good = gap == 0
        for j in range(slash_ref.shape[0]):
            good = good | (gap == slash_ref[j, c])
        chosen = block == vert_ref[c, 0]
        for e in range(1, chosen_count):
            chosen = chosen | (block == vert_ref[c, e])
        good = good | (chosen & (gap > 0))
        bias = jnp.where(good & (block >= 0), 0.0, NEGATIVE)
        keys_at = lax.broadcasted_iota(jnp.int32, (rows, rows), 0)
        query_at = lax.broadcasted_iota(jnp.int32, (rows, rows), 1)
        causal = keys_at <= query_at
        scores = []
        for g in heads:
            scores.append(jnp.dot(k, qt[i, g, :HEAD_DIM], preferred_element_type=jnp.float32))
        for g, s in zip(heads, scores):
            s = jnp.concatenate(
                [s[j * BLK:(j + 1) * BLK] + bias[j:j + 1] for j in range(2 * slab_blocks)], axis=0)
            s = jnp.concatenate([s[:rows], jnp.where(causal, s[rows:], NEGATIVE)], axis=0)
            peak = jnp.max(s, axis=0, keepdims=True)
            p = jnp.exp2((s - peak) * SCALE)
            top[i, g] = peak
            total[i, g] = jnp.sum(p, axis=0, keepdims=True)
            acc[i, g] = jnp.dot(vt, p.astype(jnp.bfloat16), preferred_element_type=jnp.float32)

    def second_keys(step, _):
        for dq in (1, -1):
            second(step, dq, pass_on(0))
        return 0

    def last_ones(part):
        def one(step, _):
            second(step, 2, lambda slab, kind, ways: arrived(part, slab))
            return 0

        lax.fori_loop(0, SIDE, one, 0)

    lax.fori_loop(0, SIDE, second_keys, 0)
    turn(c)
    for dp in (1, -1, 2):
        first(dp, pass_on(1))
    for copy in next_copies():
        copy.wait_recv()
    last_ones(0)

    lane = lax.broadcasted_iota(jnp.int32, (BLK, HEAD_DIM), 1)
    limit = (o * SIDE + lane - 1) * slab_blocks
    unit = jnp.where((lane >= SIDE) & (lane < SIDE + 3), 1.0, 0.0)
    chunks = jnp.minimum(chosen_count // FAR_CHUNK, (o + 2) // 2)

    def place(e):
        slab = vert_ref[c, e] // slab_blocks
        before = jnp.where(e > 0, vert_ref[c, jnp.maximum(e - 1, 0)] // slab_blocks, -1)
        return slab * CAP + jnp.where(before == slab, 1, 0)

    def collect_keys(n, _):
        for j in range(8):
            e = n * 8 + j
            at_row = pl.ds(pl.multiple_of(e * BLK, BLK), BLK)
            kc[at_row, :HEAD_DIM] = slots[0][place(e)]
            mask = jnp.where((lane < SIDE) & (vert_ref[c, e] >= limit), NEGATIVE, unit)
            kc[at_row, HEAD_DIM:] = mask.astype(jnp.bfloat16)
        return 0

    def collect_values(n, _):
        for j in range(4):
            pair = n * 4 + j
            both = jnp.concatenate([slots[1][place(pair * 2)], slots[1][place(pair * 2 + 1)]], axis=0)
            vtc[pair] = both.T
        return 0

    def keys_of(n):
        return kc[pl.ds(pl.multiple_of(n * FAR_CHUNK * BLK, FAR_CHUNK * BLK), FAR_CHUNK * BLK), :]

    def largest(i):
        def chunk(n, peaks):
            k = keys_of(n)
            return tuple(
                jnp.maximum(peak, jnp.max(jnp.dot(k, qt[i, g], preferred_element_type=jnp.float32),
                                          axis=0, keepdims=True))
                for g, peak in zip(heads, peaks))

        near_peaks = tuple(top[i, g] for g in heads)
        peaks = lax.fori_loop(0, chunks, chunk, near_peaks)
        row = lax.broadcasted_iota(jnp.int32, (AUX, rows), 0)
        for g, peak, old in zip(heads, peaks, near_peaks):
            shrink = jnp.exp2((old - peak) * SCALE)
            total[i, g] = total[i, g] * shrink
            acc[i, g] = acc[i, g] * shrink
            rest = -peak
            aux = jnp.where(row == i, 1.0, 0.0)
            for j in range(3):
                part = rest.astype(jnp.bfloat16).astype(jnp.float32)
                aux = jnp.where(row == SIDE + j, part, aux)
                rest = rest - part
            qt[i, g, HEAD_DIM:HEAD_DIM + AUX] = aux.astype(jnp.bfloat16)

    lax.fori_loop(0, chunks * (FAR_CHUNK // 8), collect_keys, 0)

    def first_pass(step, _):
        i = (c + step) % SIDE

        @pl.when(step > 0)
        def _():
            remote(qg.at[i], qg.at[i], q_send.at[1], q_recv.at[i], next_plane).wait_recv()
            turn(i)

        for dq in (1, -1):
            second(step, dq, pass_on(1))
        near(i)
        largest(i)
        return 0

    lax.fori_loop(0, SIDE, first_pass, 0)
    last_ones(1)
    lax.fori_loop(0, chunks * (FAR_CHUNK // 8), collect_values, 0)

    def o_copy(i, to):
        return remote(o_buf.at[i], attn.at[c], o_send.at[i], o_recv.at[c], o * SIDE + to)

    def far_slab(step, _):
        i = (c + SIDE - 1 - step) % SIDE

        def chunk(n, _):
            k = keys_of(n)
            vt = jnp.concatenate([vtc[n * (FAR_CHUNK // 2) + j] for j in range(FAR_CHUNK // 2)], axis=1)
            for g in heads:
                s = jnp.dot(k, qt[i, g], preferred_element_type=jnp.float32)
                p = jnp.exp2(s * SCALE)
                total[i, g] += jnp.sum(p, axis=0, keepdims=True)
                acc[i, g] += jnp.dot(vt, p.astype(jnp.bfloat16), preferred_element_type=jnp.float32)
            return 0

        lax.fori_loop(0, chunks, chunk, 0)
        for g in heads:
            a = acc[i, g] * (1.0 / total[i, g])
            o_buf[i, :, g * HEAD_DIM:(g + 1) * HEAD_DIM] = a.T.astype(jnp.bfloat16)

        @pl.when(step < SIDE - 1)
        def _():
            o_copy(i, i).start()

        return 0

    lax.fori_loop(0, SIDE, far_slab, 0)
    attn[c] = o_buf[c]
    for d in range(1, SIDE):
        there = attn.at[peer(d)]
        remote(there, there, o_send.at[peer(d)], o_recv.at[peer(d)], next_plane).wait_recv()

    weight_copy.wait()
    tiles = give.shape[0]
    mine = pl.ds(pl.multiple_of(core * half, half), half)
    theirs = pl.ds(pl.multiple_of(other * half, half), half)

    def swap(t):
        return pltpu.make_async_remote_copy(
            src_ref=give.at[t], dst_ref=take.at[t], send_sem=x_send.at[t], recv_sem=x_recv.at[t],
            device_id=(me, other), device_id_type=MESH,
        )

    def project(t, _):
        columns = pl.ds(pl.multiple_of(t * tile, tile), tile)
        a = jnp.concatenate([attn[j] for j in range(SIDE)], axis=1)
        res[t] = jnp.dot(a, w_ref[:, columns], preferred_element_type=jnp.float32)
        give[t] = res[t, theirs, :].astype(jnp.bfloat16)
        swap(t).start()
        return 0

    lax.fori_loop(0, tiles, project, 0)

    def add_up(t, _):
        columns = pl.ds(pl.multiple_of(t * tile, tile), tile)
        swap(t).wait_recv()
        out_ref[:, columns] = (res[t, mine, :] + take[t].astype(jnp.float32)).astype(out_ref.dtype)
        return 0

    lax.fori_loop(0, tiles, add_up, 0)

    def swapped(t, _):
        swap(t).wait_send()
        return 0

    lax.fori_loop(0, tiles, swapped, 0)
    for d in range(1, SIDE):
        for part in range(2):
            pack_copy(part, d).wait_send()
        for copy in kv_copies(d):
            copy.wait_send()
        q_copy(d).wait_send()
        o_copy(peer(d), peer(d)).wait_send()
    for copy in next_copies():
        copy.wait_send()
    for part in range(2):
        own(sent(part))
        for dp in (1, -1, 2):
            first(dp, sent(part))

    def ring_sent(step, _):
        for part in range(2):
            for dq in (1, -1):
                second(step, dq, sent(part))
        return 0

    lax.fori_loop(0, SIDE, ring_sent, 0)


def on_device(n, queries, keys, values, vertical, slash, out_weight):
    rows = queries.shape[0]
    kv = vertical.shape[0]
    per_group = queries.shape[1] // (kv * HEAD_DIM)
    width = per_group * HEAD_DIM
    model = out_weight.shape[1]
    listed = vertical.shape[1]

    tile = math.gcd(model, 512)
    tiles = model // tile
    vmem = pl.BlockSpec(memory_space=pltpu.VMEM)
    smem = pl.BlockSpec(memory_space=pltpu.SMEM)
    dma = pltpu.SemaphoreType.DMA
    return pl.pallas_call(
        functools.partial(kernel, per_group, tile),
        out_shape=jax.ShapeDtypeStruct((rows // 2, model), jnp.bfloat16),
        in_specs=[vmem] * 3 + [smem] * 2 + [pl.BlockSpec(memory_space=pl.ANY)],
        out_specs=vmem,
        scratch_shapes=[
            [pltpu.VMEM((kv, CAP, BLK, HEAD_DIM), jnp.bfloat16) for _ in range(2)],
            [pltpu.VMEM((n * CAP, BLK, HEAD_DIM), jnp.bfloat16) for _ in range(2)],
            pltpu.VMEM((SIDE, rows, width), jnp.bfloat16),
            pltpu.VMEM((SIDE, per_group, 2 * HEAD_DIM, rows), jnp.bfloat16),
            pltpu.VMEM((SIDE + 1, rows, HEAD_DIM), jnp.bfloat16),
            pltpu.VMEM((SIDE + 1, rows, HEAD_DIM), jnp.bfloat16),
            pltpu.VMEM((listed * BLK, 2 * HEAD_DIM), jnp.bfloat16),
            pltpu.VMEM((listed // 2, HEAD_DIM, 2 * BLK), jnp.bfloat16),
            pltpu.VMEM(out_weight.shape, jnp.bfloat16),
            pltpu.VMEM((SIDE, per_group, HEAD_DIM, rows), jnp.float32),
            pltpu.VMEM((SIDE, per_group, 1, rows), jnp.float32),
            pltpu.VMEM((SIDE, per_group, 1, rows), jnp.float32),
            pltpu.VMEM((SIDE, rows, width), jnp.bfloat16),
            pltpu.VMEM((SIDE, rows, width), jnp.bfloat16),
            pltpu.VMEM((tiles, rows, tile), jnp.float32),
            pltpu.VMEM((tiles, rows // 2, tile), jnp.bfloat16),
            pltpu.VMEM((tiles, rows // 2, tile), jnp.bfloat16),
            dma,
            dma((2, SIDE)),
            dma((SIDE, 2)),
            dma((SIDE + 1, 2)),
            dma((SIDE,)),
            dma((SIDE,)),
            dma((2, n)),
            dma((2, n, SIDE)),
            dma((SIDE,)),
            dma((SIDE,)),
            dma((tiles,)),
            dma((tiles,)),
        ],
        compiler_params=pltpu.CompilerParams(
            collective_id=0, has_side_effects=True, vmem_limit_bytes=60 * 2**20
        ),
    )(queries, keys, values, vertical, slash.T, out_weight)


def solution(mesh):
    placed = (
        P("seq", "head"),
        P("seq", "head"),
        P("seq", "head"),
        P("head", None),
        P("head", None),
        P("head", None),
    )
    return jax.shard_map(
        functools.partial(on_device, mesh.shape["seq"]),
        mesh=mesh, in_specs=placed, out_specs=P(("seq", "head"), None), check_vma=False,
    )
```

```python
import functools
import math

import jax
import jax.numpy as jnp
from jax import lax
from jax.experimental import pallas as pl
from jax.experimental.pallas import tpu as pltpu
from jax.sharding import PartitionSpec as P

HEAD_DIM = 128
BLK = 64
CAP = 2
NEGATIVE = -1e30
MESH = pl.DeviceIdType.MESH
SCALE = HEAD_DIM ** (-0.5) * math.log2(math.e)
SIDE = 4
FAR_CHUNK = 16
AUX = 16


def kernel(
    per_group, tile,
    q_ref, k_ref, v_ref, vert_ref, slash_ref, w_hbm, out_ref,
    packs, slots, qg, qt, kg, vg, kc, vtc, w_ref, acc, top, total, o_buf, attn, res, give, take,
    w_sem, pack_send, kv_send, kv_recv, q_send, q_recv, slot_recv, ring_send,
    o_send, o_recv, x_send, x_recv,
):
    rows = q_ref.shape[0]
    me = lax.axis_index("seq")
    core = lax.axis_index("head")
    other = 1 - core
    o, c = me // SIDE, me % SIDE
    x, z = o // SIDE, o % SIDE
    slab_blocks = rows // BLK
    half = rows // 2
    width = per_group * HEAD_DIM
    chosen_count = vert_ref.shape[1]
    next_plane = (me + SIDE) % (SIDE ** 3)
    last_plane = (me + SIDE ** 3 - SIDE) % (SIDE ** 3)

    def at(xx, zz, cc):
        return (xx % SIDE * SIDE + zz % SIDE) * SIDE + cc

    barrier = pltpu.get_barrier_semaphore()

    def greet(seq, head):
        pl.semaphore_signal(barrier, inc=1, device_id=(seq, head), device_id_type=MESH)

    greet(me, other)
    for d in range(1, SIDE):
        greet(o * SIDE + (c + d) % SIDE, core)
    for step in (1, SIDE - 1):
        greet(at(x + step, z, c), core)
        greet(at(x, z + step, c), core)
    greet(next_plane, core)
    greet(last_plane, core)

    weight_copy = pltpu.make_async_copy(w_hbm, w_ref, w_sem)
    weight_copy.start()

    def lanes(h, size=HEAD_DIM):
        return pl.ds(pl.multiple_of(h * size, size), size)

    first_block = me * slab_blocks
    for h in range(SIDE):
        low, high = jnp.int32(slab_blocks), jnp.int32(-1)
        for e in range(chosen_count):
            block = vert_ref[h, e] - first_block
            inside = (block >= 0) & (block < slab_blocks)
            low = jnp.where(inside, jnp.minimum(low, block), low)
            high = jnp.where(inside, jnp.maximum(high, block), high)
        for slot, block in enumerate((low, high)):
            for part, source in enumerate((k_ref, v_ref)):
                got = source[:BLK, h * HEAD_DIM:(h + 1) * HEAD_DIM]
                for i in range(1, slab_blocks):
                    rows_i = source[i * BLK:(i + 1) * BLK, h * HEAD_DIM:(h + 1) * HEAD_DIM]
                    got = jnp.where(block == i, rows_i, got)
                packs[part][h, slot] = got
    for part in range(2):
        for i in range(CAP):
            slots[part][me * CAP + i] = packs[part][c, i]
    kg[c + 1] = k_ref[:, lanes(c)]
    vg[c + 1] = v_ref[:, lanes(c)]
    qg[c] = q_ref[:, lanes(c, width)]

    pl.semaphore_wait(barrier, 1 + (SIDE - 1) + 4 + 2)

    def remote(src, dst, send_sem, recv_sem, seq):
        return pltpu.make_async_remote_copy(
            src_ref=src, dst_ref=dst, send_sem=send_sem, recv_sem=recv_sem,
            device_id=(seq, core), device_id_type=MESH,
        )

    def held(part, slab):
        return slots[part].at[pl.ds(slab * CAP, CAP)]

    def peer(d):
        return (c + d) % SIDE

    def pack_copy(part, d):
        return remote(packs[part].at[peer(d)], held(part, me), pack_send.at[part, d], slot_recv.at[part, me],
                      o * SIDE + peer(d))

    def kv_copies(d):
        to = peer(d)
        return [
            remote(source.at[:, lanes(to)], got.at[c + 1], kv_send.at[d, i], kv_recv.at[c + 1, i], o * SIDE + to)
            for i, (source, got) in enumerate(((k_ref, kg), (v_ref, vg)))
        ]

    def q_copy(d):
        to = peer(d)
        return remote(q_ref.at[:, lanes(to, width)], qg.at[c], q_send.at[d], q_recv.at[c], o * SIDE + to)

    def next_copies():
        return [
            remote(got.at[SIDE], got.at[0], kv_send.at[0, i], kv_recv.at[0, i], next_plane)
            for i, got in enumerate((kg, vg))
        ]

    near_order = (1, SIDE - 1, 2)
    for part in range(2):
        for d in near_order:
            pack_copy(part, d).start()
    for d in near_order:
        for copy in kv_copies(d):
            copy.start()
    for d in near_order:
        q_copy(d).start()

    def slab_of(dp, dq, kind):
        dx, dz = (dp, dq) if kind < 2 else (dq, dp)
        return at(x + SIDE - dx, z + SIDE - dz, kind)

    def ring(part, slab, kind, phase, sign):
        x_first = kind < 2
        along_x = x_first if phase == 0 else jnp.logical_not(x_first)
        to = jnp.where(along_x, at(x + SIDE + sign, z, c), at(x, z + SIDE + sign, c))
        there = held(part, slab)
        return remote(there, there, ring_send.at[part], slot_recv.at[part, slab], to)

    def arrived(part, slab):
        there = held(part, slab)
        remote(there, there, pack_send.at[part, 1], slot_recv.at[part, slab], next_plane).wait_recv()

    def sign_of(kind):
        return 1 if kind % 2 == 0 else -1

    def first(dp, act):
        for kind in range(SIDE):
            ways = [(0, dp)] if dp == sign_of(kind) else []
            act(slab_of(dp, 0, kind), kind, ways + [(1, 1), (1, -1)])

    def second(dp, dq, act):
        for kind in range(SIDE):
            act(slab_of(dp, dq, kind), kind, [(1, dq)] if dq == sign_of(kind) else [])

    def pass_on(part):
        def act(slab, kind, ways):
            arrived(part, slab)
            for phase, sign in ways:
                ring(part, slab, kind, phase, sign).start()

        return act

    def pass_own(part):
        for d in (0, SIDE - 1, 1, 2):
            slab = o * SIDE + peer(d)
            if d:
                arrived(part, slab)
            for phase, sign in ((0, 1), (0, -1), (1, 1), (1, -1)):
                ring(part, slab, peer(d), phase, sign).start()

    pass_own(0)
    for dp in (1, -1, 2):
        first(dp, pass_on(0))

    for d in range(1, SIDE):
        for i, got in enumerate((kg, vg)):
            there = got.at[peer(d) + 1]
            remote(there, there, kv_send.at[d, i], kv_recv.at[peer(d) + 1, i], next_plane).wait_recv()
    for copy in next_copies():
        copy.start()

    heads = range(per_group)

    def turn(i):
        row = lax.broadcasted_iota(jnp.int32, (HEAD_DIM, rows), 0)
        for g in heads:
            qt[i, g, :HEAD_DIM] = qg[i, :, g * HEAD_DIM:(g + 1) * HEAD_DIM].T
            qt[i, g, HEAD_DIM:] = jnp.where(row == i, 1.0, 0.0).astype(jnp.bfloat16)

    def near(i):
        base = (o * SIDE + i) * slab_blocks
        k = jnp.concatenate([kg[i], kg[i + 1]], axis=0)
        vt = jnp.concatenate([vg[i], vg[i + 1]], axis=0).T
        shape = (2 * slab_blocks, rows)
        block = lax.broadcasted_iota(jnp.int32, shape, 0) - slab_blocks
        gap = lax.broadcasted_iota(jnp.int32, shape, 1) // BLK - block
        block = base + block
        good = gap == 0
        for j in range(slash_ref.shape[0]):
            good = good | (gap == slash_ref[j, c])
        chosen = block == vert_ref[c, 0]
        for e in range(1, chosen_count):
            chosen = chosen | (block == vert_ref[c, e])
        good = good | (chosen & (gap > 0))
        bias = jnp.where(good & (block >= 0), 0.0, NEGATIVE)
        keys_at = lax.broadcasted_iota(jnp.int32, (rows, rows), 0)
        query_at = lax.broadcasted_iota(jnp.int32, (rows, rows), 1)
        causal = keys_at <= query_at
        scores = []
        for g in heads:
            scores.append(jnp.dot(k, qt[i, g, :HEAD_DIM], preferred_element_type=jnp.float32))
        for g, s in zip(heads, scores):
            s = jnp.concatenate(
                [s[j * BLK:(j + 1) * BLK] + bias[j:j + 1] for j in range(2 * slab_blocks)], axis=0)
            s = jnp.concatenate([s[:rows], jnp.where(causal, s[rows:], NEGATIVE)], axis=0)
            peak = jnp.max(s, axis=0, keepdims=True)
            p = jnp.exp2((s - peak) * SCALE)
            top[i, g] = peak
            total[i, g] = jnp.sum(p, axis=0, keepdims=True)
            acc[i, g] = jnp.dot(vt, p.astype(jnp.bfloat16), preferred_element_type=jnp.float32)

    def second_keys(step, _):
        for dq in (1, -1):
            second(step, dq, pass_on(0))
        return 0

    def last_ones(part):
        def one(step, _):
            second(step, 2, lambda slab, kind, ways: arrived(part, slab))
            return 0

        lax.fori_loop(0, SIDE, one, 0)

    lax.fori_loop(0, SIDE, second_keys, 0)
    pass_own(1)
    turn(c)
    for copy in next_copies():
        copy.wait_recv()
    near(c)
    last_ones(0)

    lane = lax.broadcasted_iota(jnp.int32, (BLK, HEAD_DIM), 1)
    limit = (o * SIDE + lane - 1) * slab_blocks
    unit = jnp.where((lane >= SIDE) & (lane < SIDE + 3), 1.0, 0.0)
    chunks = jnp.minimum(chosen_count // FAR_CHUNK, (o + 2) // 2)

    def place(e):
        slab = vert_ref[c, e] // slab_blocks
        before = jnp.where(e > 0, vert_ref[c, jnp.maximum(e - 1, 0)] // slab_blocks, -1)
        return slab * CAP + jnp.where(before == slab, 1, 0)

    def collect_keys(n, _):
        for j in range(8):
            e = n * 8 + j
            at_row = pl.ds(pl.multiple_of(e * BLK, BLK), BLK)
            kc[at_row, :HEAD_DIM] = slots[0][place(e)]
            mask = jnp.where((lane < SIDE) & (vert_ref[c, e] >= limit), NEGATIVE, unit)
            kc[at_row, HEAD_DIM:] = mask.astype(jnp.bfloat16)
        return 0

    def collect_values(n, _):
        for j in range(4):
            pair = n * 4 + j
            both = jnp.concatenate([slots[1][place(pair * 2)], slots[1][place(pair * 2 + 1)]], axis=0)
            vtc[pair] = both.T
        return 0

    def keys_of(n):
        return kc[pl.ds(pl.multiple_of(n * FAR_CHUNK * BLK, FAR_CHUNK * BLK), FAR_CHUNK * BLK), :]

    def largest(i):
        def chunk(n, peaks):
            k = keys_of(n)
            return tuple(
                jnp.maximum(peak, jnp.max(jnp.dot(k, qt[i, g], preferred_element_type=jnp.float32),
                                          axis=0, keepdims=True))
                for g, peak in zip(heads, peaks))

        near_peaks = tuple(top[i, g] for g in heads)
        peaks = lax.fori_loop(0, chunks, chunk, near_peaks)
        row = lax.broadcasted_iota(jnp.int32, (AUX, rows), 0)
        for g, peak, old in zip(heads, peaks, near_peaks):
            shrink = jnp.exp2((old - peak) * SCALE)
            total[i, g] = total[i, g] * shrink
            acc[i, g] = acc[i, g] * shrink
            rest = -peak
            aux = jnp.where(row == i, 1.0, 0.0)
            for j in range(3):
                part = rest.astype(jnp.bfloat16).astype(jnp.float32)
                aux = jnp.where(row == SIDE + j, part, aux)
                rest = rest - part
            qt[i, g, HEAD_DIM:HEAD_DIM + AUX] = aux.astype(jnp.bfloat16)

    lax.fori_loop(0, chunks * (FAR_CHUNK // 8), collect_keys, 0)

    def first_pass(step, _):
        i = (c + step) % SIDE

        @pl.when(step > 0)
        def _():
            remote(qg.at[i], qg.at[i], q_send.at[1], q_recv.at[i], next_plane).wait_recv()
            turn(i)
            near(i)

        largest(i)

        @pl.when(step == 0)
        def _():
            for dp in (1, -1):
                first(dp, pass_on(1))

        @pl.when(step == 1)
        def _():
            first(2, pass_on(1))
            for dq in (1, -1):
                second(0, dq, pass_on(1))

        @pl.when(step == 2)
        def _():
            def rest(dp, _):
                for dq in (1, -1):
                    second(dp, dq, pass_on(1))
                return 0

            lax.fori_loop(1, SIDE, rest, 0)

        return 0

    lax.fori_loop(0, SIDE, first_pass, 0)
    last_ones(1)
    lax.fori_loop(0, chunks * (FAR_CHUNK // 8), collect_values, 0)

    def o_copy(i, to):
        return remote(o_buf.at[i], attn.at[c], o_send.at[i], o_recv.at[c], o * SIDE + to)

    def far_slab(step, _):
        i = (c + SIDE - 1 - step) % SIDE

        def chunk(n, _):
            k = keys_of(n)
            vt = jnp.concatenate([vtc[n * (FAR_CHUNK // 2) + j] for j in range(FAR_CHUNK // 2)], axis=1)
            scores = [jnp.dot(k, qt[i, g], preferred_element_type=jnp.float32) for g in heads]
            old = [(total[i, g], acc[i, g]) for g in heads]
            new = []
            for s, (amount, mix) in zip(scores, old):
                p = jnp.exp2(s * SCALE)
                amount = amount + jnp.sum(p, axis=0, keepdims=True)
                mix = mix + jnp.dot(vt, p.astype(jnp.bfloat16), preferred_element_type=jnp.float32)
                new.append((amount, mix))
            for g, (amount, mix) in zip(heads, new):
                total[i, g] = amount
                acc[i, g] = mix
            return 0

        lax.fori_loop(0, chunks, chunk, 0)
        for g in heads:
            a = acc[i, g] * (1.0 / total[i, g])
            o_buf[i, :, g * HEAD_DIM:(g + 1) * HEAD_DIM] = a.T.astype(jnp.bfloat16)

        @pl.when(step < SIDE - 1)
        def _():
            o_copy(i, i).start()

        return 0

    lax.fori_loop(0, SIDE, far_slab, 0)
    attn[c] = o_buf[c]
    for d in range(1, SIDE):
        there = attn.at[peer(d)]
        remote(there, there, o_send.at[peer(d)], o_recv.at[peer(d)], next_plane).wait_recv()

    weight_copy.wait()
    tiles = give.shape[0]
    mine = pl.ds(pl.multiple_of(core * half, half), half)
    theirs = pl.ds(pl.multiple_of(other * half, half), half)

    def swap(t):
        return pltpu.make_async_remote_copy(
            src_ref=give.at[t], dst_ref=take.at[t], send_sem=x_send.at[t], recv_sem=x_recv.at[t],
            device_id=(me, other), device_id_type=MESH,
        )

    def project(t, _):
        columns = pl.ds(pl.multiple_of(t * tile, tile), tile)
        a = jnp.concatenate([attn[j] for j in range(SIDE)], axis=1)
        res[t] = jnp.dot(a, w_ref[:, columns], preferred_element_type=jnp.float32)
        give[t] = res[t, theirs, :].astype(jnp.bfloat16)
        swap(t).start()
        return 0

    lax.fori_loop(0, tiles, project, 0)

    def add_up(t, _):
        columns = pl.ds(pl.multiple_of(t * tile, tile), tile)
        swap(t).wait_recv()
        out_ref[:, columns] = (res[t, mine, :] + take[t].astype(jnp.float32)).astype(out_ref.dtype)
        return 0

    lax.fori_loop(0, tiles, add_up, 0)

    def swapped(t, _):
        swap(t).wait_send()
        return 0

    lax.fori_loop(0, tiles, swapped, 0)
    for d in range(1, SIDE):
        for part in range(2):
            pack_copy(part, d).wait_send()
        for copy in kv_copies(d):
            copy.wait_send()
        q_copy(d).wait_send()
        o_copy(peer(d), peer(d)).wait_send()
    for copy in next_copies():
        copy.wait_send()
    for part in range(2):
        every = slots[part].at[pl.ds(0, (SIDE ** 3 - SIDE) * CAP)]
        remote(every, every, ring_send.at[part], slot_recv.at[part, 0], next_plane).wait_send()


def on_device(n, queries, keys, values, vertical, slash, out_weight):
    rows = queries.shape[0]
    kv = vertical.shape[0]
    per_group = queries.shape[1] // (kv * HEAD_DIM)
    width = per_group * HEAD_DIM
    model = out_weight.shape[1]
    listed = vertical.shape[1]

    tile = math.gcd(model, 1024)
    tiles = model // tile
    vmem = pl.BlockSpec(memory_space=pltpu.VMEM)
    smem = pl.BlockSpec(memory_space=pltpu.SMEM)
    dma = pltpu.SemaphoreType.DMA
    return pl.pallas_call(
        functools.partial(kernel, per_group, tile),
        out_shape=jax.ShapeDtypeStruct((rows // 2, model), jnp.bfloat16),
        in_specs=[vmem] * 3 + [smem] * 2 + [pl.BlockSpec(memory_space=pl.ANY)],
        out_specs=vmem,
        scratch_shapes=[
            [pltpu.VMEM((kv, CAP, BLK, HEAD_DIM), jnp.bfloat16) for _ in range(2)],
            [pltpu.VMEM((n * CAP, BLK, HEAD_DIM), jnp.bfloat16) for _ in range(2)],
            pltpu.VMEM((SIDE, rows, width), jnp.bfloat16),
            pltpu.VMEM((SIDE, per_group, 2 * HEAD_DIM, rows), jnp.bfloat16),
            pltpu.VMEM((SIDE + 1, rows, HEAD_DIM), jnp.bfloat16),
            pltpu.VMEM((SIDE + 1, rows, HEAD_DIM), jnp.bfloat16),
            pltpu.VMEM((listed * BLK, 2 * HEAD_DIM), jnp.bfloat16),
            pltpu.VMEM((listed // 2, HEAD_DIM, 2 * BLK), jnp.bfloat16),
            pltpu.VMEM(out_weight.shape, jnp.bfloat16),
            pltpu.VMEM((SIDE, per_group, HEAD_DIM, rows), jnp.float32),
            pltpu.VMEM((SIDE, per_group, 1, rows), jnp.float32),
            pltpu.VMEM((SIDE, per_group, 1, rows), jnp.float32),
            pltpu.VMEM((SIDE, rows, width), jnp.bfloat16),
            pltpu.VMEM((SIDE, rows, width), jnp.bfloat16),
            pltpu.VMEM((tiles, rows, tile), jnp.float32),
            pltpu.VMEM((tiles, rows // 2, tile), jnp.bfloat16),
            pltpu.VMEM((tiles, rows // 2, tile), jnp.bfloat16),
            dma,
            dma((2, SIDE)),
            dma((SIDE, 2)),
            dma((SIDE + 1, 2)),
            dma((SIDE,)),
            dma((SIDE,)),
            dma((2, n)),
            dma((2,)),
            dma((SIDE,)),
            dma((SIDE,)),
            dma((tiles,)),
            dma((tiles,)),
        ],
        compiler_params=pltpu.CompilerParams(
            collective_id=0, has_side_effects=True, vmem_limit_bytes=60 * 2**20
        ),
    )(queries, keys, values, vertical, slash.T, out_weight)


def solution(mesh):
    placed = (
        P("seq", "head"),
        P("seq", "head"),
        P("seq", "head"),
        P("head", None),
        P("head", None),
        P("head", None),
    )
    return jax.shard_map(
        functools.partial(on_device, mesh.shape["seq"]),
        mesh=mesh, in_specs=placed, out_specs=P(("seq", "head"), None), check_vma=False,
    )
```

```python
import functools
import math

import jax
import jax.numpy as jnp
from jax import lax
from jax.experimental import pallas as pl
from jax.experimental.pallas import tpu as pltpu
from jax.sharding import PartitionSpec as P

HEAD_DIM = 128
BLK = 64
CAP = 2
NEGATIVE = -1e30
MESH = pl.DeviceIdType.MESH
SCALE = HEAD_DIM ** (-0.5) * math.log2(math.e)
SIDE = 4
FAR_CHUNK = 32
PAIRS = 2
FAR_PARTS = 2
TOP_CHUNK = 32
AUX = 16


def kernel(
    per_group, tile,
    q_ref, k_ref, v_ref, list_ref, vert_ref, slash_ref, w_hbm, out_ref,
    packs, slots, qg, qt, kg, vg, aux_k, places, w_ref, acc, top, far_top, total, o_buf, attn, res, give, take, out_buf,
    w_sem, pack_send, kv_send, kv_recv, q_send, q_recv, slot_recv, ring_send,
    o_send, o_recv, x_send, x_recv, out_sem,
):
    rows = q_ref.shape[0]
    me = lax.axis_index("seq")
    core = lax.axis_index("head")
    other = 1 - core
    o, c = me // SIDE, me % SIDE
    x, z = o // SIDE, o % SIDE
    slab_blocks = rows // BLK
    half = rows // 2
    width = per_group * HEAD_DIM
    chosen_count = vert_ref.shape[1]
    next_plane = (me + SIDE) % (SIDE ** 3)
    last_plane = (me + SIDE ** 3 - SIDE) % (SIDE ** 3)

    def at(xx, zz, cc):
        return (xx % SIDE * SIDE + zz % SIDE) * SIDE + cc

    barrier = pltpu.get_barrier_semaphore()

    def greet(seq, head):
        pl.semaphore_signal(barrier, inc=1, device_id=(seq, head), device_id_type=MESH)

    greet(me, other)
    for d in range(1, SIDE):
        greet(o * SIDE + (c + d) % SIDE, core)
    for step in range(1, SIDE):
        greet(at(x + step, z, c), core)
        greet(at(x, z + step, c), core)
    greet(next_plane, core)
    greet(last_plane, core)

    weight_copy = pltpu.make_async_copy(w_hbm, w_ref, w_sem)
    weight_copy.start()

    def lanes(h, size=HEAD_DIM):
        return pl.ds(pl.multiple_of(h * size, size), size)

    first_block = me * slab_blocks
    found = list_ref[...] - first_block
    inside = (found >= 0) & (found < slab_blocks)
    low = jnp.min(jnp.where(inside, found, slab_blocks), axis=1, keepdims=True)
    high = jnp.max(jnp.where(inside, found, -1), axis=1, keepdims=True)
    for h in range(SIDE):
        for slot, extreme in enumerate((low, high)):
            pick = jnp.broadcast_to(extreme[h:h + 1], (BLK, HEAD_DIM))
            for part, source in enumerate((k_ref, v_ref)):
                got = source[:BLK, h * HEAD_DIM:(h + 1) * HEAD_DIM]
                for i in range(1, slab_blocks):
                    rows_i = source[i * BLK:(i + 1) * BLK, h * HEAD_DIM:(h + 1) * HEAD_DIM]
                    got = jnp.where(pick == i, rows_i, got)
                packs[part][h, slot] = got
    for part in range(2):
        for i in range(CAP):
            slots[part][me * CAP + i] = packs[part][c, i]
    kg[c + 1] = k_ref[:, lanes(c)]
    vg[c + 1] = v_ref[:, lanes(c)]
    qg[c] = q_ref[:, lanes(c, width)]

    pl.semaphore_wait(barrier, 1 + 3 * (SIDE - 1) + 2)

    def remote(src, dst, send_sem, recv_sem, seq):
        return pltpu.make_async_remote_copy(
            src_ref=src, dst_ref=dst, send_sem=send_sem, recv_sem=recv_sem,
            device_id=(seq, core), device_id_type=MESH,
        )

    def held(part, slab):
        return slots[part].at[pl.ds(slab * CAP, CAP)]

    def peer(d):
        return (c + d) % SIDE

    def pack_copy(part, d):
        return remote(packs[part].at[peer(d)], held(part, me), pack_send.at[part, d], slot_recv.at[part, me],
                      o * SIDE + peer(d))

    def kv_copies(d):
        to = peer(d)
        return [
            remote(source.at[:, lanes(to)], got.at[c + 1], kv_send.at[d, i], kv_recv.at[c + 1, i], o * SIDE + to)
            for i, (source, got) in enumerate(((k_ref, kg), (v_ref, vg)))
        ]

    def q_copy(d):
        to = peer(d)
        return remote(q_ref.at[:, lanes(to, width)], qg.at[c], q_send.at[d], q_recv.at[c], o * SIDE + to)

    def next_copies():
        return [
            remote(got.at[SIDE], got.at[0], kv_send.at[0, i], kv_recv.at[0, i], next_plane)
            for i, got in enumerate((kg, vg))
        ]

    near_order = (1, SIDE - 1, 2)
    for d in near_order:
        pack_copy(0, d).start()

    def slab_of(dp, dq, kind):
        x_first = kind < 2
        return jnp.where(x_first, at(x + SIDE - dp, z + SIDE - dq, kind), at(x + SIDE - dq, z + SIDE - dp, kind))

    def ring(part, slab, kind, phase, sign):
        x_first = kind < 2
        along_x = x_first if phase == 0 else jnp.logical_not(x_first)
        to = jnp.where(along_x, at(x + SIDE + sign, z, c), at(x, z + SIDE + sign, c))
        there = held(part, slab)
        return remote(there, there, ring_send.at[part], slot_recv.at[part, slab], to)

    def arrived(part, slab):
        there = held(part, slab)
        remote(there, there, pack_send.at[part, 1], slot_recv.at[part, slab], next_plane).wait_recv()

    def sign_of(kind):
        return 1 if kind % 2 == 0 else -1

    def first(act):
        for d in (0, SIDE - 1, 1, 2):
            for dp in (1, -1, 2):
                act(slab_of(dp, 0, peer(d)), peer(d), [(1, 1), (1, -1)])

    def second(dp, dq, act):
        for kind in range(SIDE):
            act(slab_of(dp, dq, kind), kind, [(1, dq)] if dq == sign_of(kind) else [])

    def pass_on(part):
        def act(slab, kind, ways):
            arrived(part, slab)
            for phase, sign in ways:
                ring(part, slab, kind, phase, sign).start()

        return act

    def pass_own(part):
        for d in (0, SIDE - 1, 1, 2):
            slab = o * SIDE + peer(d)
            if d:
                arrived(part, slab)
            for phase, sign in ((0, 1), (0, -1), (0, 2), (1, 1), (1, -1)):
                ring(part, slab, peer(d), phase, sign).start()

    pass_own(0)
    for d in near_order:
        for copy in kv_copies(d):
            copy.start()
    for d in near_order:
        pack_copy(1, d).start()
    for d in (SIDE - 1, 1, 2):
        q_copy(d).start()
    lane = lax.broadcasted_iota(jnp.int32, (BLK, HEAD_DIM), 1)
    limit = (o * SIDE + lane - 1) * slab_blocks
    unit = jnp.where((lane >= SIDE) & (lane < SIDE + 3), 1.0, 0.0)

    def look_up(n, _):
        for j in range(8):
            e = n * 8 + j
            block = vert_ref[c, e]
            slab = block // slab_blocks
            before = jnp.where(e > 0, vert_ref[c, jnp.maximum(e - 1, 0)] // slab_blocks, -1)
            places[e] = slab * CAP + jnp.where(before == slab, 1, 0)
            mask = jnp.where((lane < SIDE) & (block >= limit), NEGATIVE, unit)
            aux_k[pl.ds(pl.multiple_of(e * BLK, BLK), BLK), :] = mask.astype(jnp.bfloat16)
        return 0

    lax.fori_loop(0, chosen_count // 8, look_up, 0)
    first(pass_on(0))

    heads = range(per_group)

    def turn(i):
        row = lax.broadcasted_iota(jnp.int32, (HEAD_DIM, rows), 0)
        for g in heads:
            qt[i, g, :HEAD_DIM] = qg[i, :, g * HEAD_DIM:(g + 1) * HEAD_DIM].T
            qt[i, g, HEAD_DIM:] = jnp.where(row == i, 1.0, 0.0).astype(jnp.bfloat16)

    def near(i):
        base = (o * SIDE + i) * slab_blocks
        k = jnp.concatenate([kg[i], kg[i + 1]], axis=0)
        vt = jnp.concatenate([vg[i], vg[i + 1]], axis=0).T
        shape = (2 * slab_blocks, rows)
        block = lax.broadcasted_iota(jnp.int32, shape, 0) - slab_blocks
        gap = lax.broadcasted_iota(jnp.int32, shape, 1) // BLK - block
        block = base + block
        good = gap == 0
        for j in range(slash_ref.shape[0]):
            good = good | (gap == slash_ref[j, c])
        chosen = block == vert_ref[c, 0]
        for e in range(1, chosen_count):
            chosen = chosen | (block == vert_ref[c, e])
        good = good | (chosen & (gap > 0))
        bias = jnp.where(good & (block >= 0), 0.0, NEGATIVE)
        keys_at = lax.broadcasted_iota(jnp.int32, (rows, rows), 0)
        query_at = lax.broadcasted_iota(jnp.int32, (rows, rows), 1)
        causal = keys_at <= query_at
        scores = []
        for g in heads:
            scores.append(jnp.dot(k, qt[i, g, :HEAD_DIM], preferred_element_type=jnp.float32))
        for g, s in zip(heads, scores):
            s = jnp.concatenate(
                [s[j * BLK:(j + 1) * BLK] + bias[j:j + 1] for j in range(2 * slab_blocks)], axis=0)
            s = jnp.concatenate([s[:rows], jnp.where(causal, s[rows:], NEGATIVE)], axis=0)
            peak = jnp.max(s, axis=0, keepdims=True)
            p = jnp.exp2((s - peak) * SCALE)
            top[i, g] = peak
            total[i, g] = jnp.sum(p, axis=0, keepdims=True)
            acc[i, g] = jnp.dot(vt, p.astype(jnp.bfloat16), preferred_element_type=jnp.float32)

    def second_keys(step, _):
        for dq in (1, -1):
            second(step, dq, pass_on(0))
        return 0

    def last_ones(part):
        def one(step, _):
            second(step, 2, lambda slab, kind, ways: arrived(part, slab))
            return 0

        lax.fori_loop(0, SIDE, one, 0)

    lax.fori_loop(0, SIDE, second_keys, 0)
    pass_own(1)
    for d in range(1, SIDE):
        for i, got in enumerate((kg, vg)):
            there = got.at[peer(d) + 1]
            remote(there, there, kv_send.at[d, i], kv_recv.at[peer(d) + 1, i], next_plane).wait_recv()
    for copy in next_copies():
        copy.start()

    def queries_in(i):
        remote(qg.at[i], qg.at[i], q_send.at[1], q_recv.at[i], next_plane).wait_recv()

    turn(c)

    @pl.when(c > 0)
    def _():
        near(c)

    last_ones(0)

    def blocks(part, n, size):
        return jnp.concatenate([slots[part][places[n * size + j]] for j in range(size)], axis=0)

    def keys_of(n, size):
        masks = aux_k[pl.ds(pl.multiple_of(n * size * BLK, size * BLK), size * BLK), :]
        return jnp.concatenate([blocks(0, n, size), masks], axis=1)

    def steps(size):
        return jnp.minimum(chosen_count, (o * SIDE + 2) * CAP + size - 1) // size

    def largest(i):
        def chunk(n, peaks):
            k = keys_of(n, TOP_CHUNK)
            return tuple(
                jnp.maximum(peak, jnp.max(jnp.dot(k, qt[i, g], preferred_element_type=jnp.float32),
                                          axis=0, keepdims=True))
                for g, peak in zip(heads, peaks))

        peaks = lax.fori_loop(0, steps(TOP_CHUNK), chunk, (jnp.full((1, rows), NEGATIVE),) * per_group)
        for g, peak in zip(heads, peaks):
            far_top[i, g] = peak

    def join(i):
        row = lax.broadcasted_iota(jnp.int32, (AUX, rows), 0)
        for g in heads:
            old = top[i, g]
            peak = jnp.maximum(old, far_top[i, g])
            shrink = jnp.exp2((old - peak) * SCALE)
            total[i, g] = total[i, g] * shrink
            acc[i, g] = acc[i, g] * shrink
            rest = -peak
            aux = jnp.where(row == i, 1.0, 0.0)
            for j in range(3):
                part = rest.astype(jnp.bfloat16).astype(jnp.float32)
                aux = jnp.where(row == SIDE + j, part, aux)
                rest = rest - part
            qt[i, g, HEAD_DIM:HEAD_DIM + AUX] = aux.astype(jnp.bfloat16)

    def first_pass(step, _):
        i = (c + step + jnp.where(step == 2, 1, jnp.where(step == 3, -1, 0))) % SIDE

        @pl.when(step > 0)
        def _():
            queries_in(i)
            turn(i)

        largest(i)

        @pl.when(step == 0)
        def _():
            first(pass_on(1))

        @pl.when(step == 2)
        def _():
            def rest(dp, _):
                for dq in (1, -1):
                    second(dp, dq, pass_on(1))
                return 0

            lax.fori_loop(0, SIDE, rest, 0)

        return 0

    lax.fori_loop(0, SIDE, first_pass, 0)
    for copy in next_copies():
        copy.wait_recv()

    def other_near(i, _):
        @pl.when((i != c) | (c == 0))
        def _():
            near(i)

        return 0

    lax.fori_loop(0, SIDE, other_near, 0)
    last_ones(1)

    def o_copies(i, pair):
        columns = pl.ds(pair * width // PAIRS, width // PAIRS)
        return remote(o_buf.at[i, :, columns], attn.at[c, :, columns], o_send.at[i, pair], o_recv.at[c, pair], o * SIDE + i)

    def far_slab(step, _):
        i = (c + SIDE - 1 - step) % SIDE
        join(i)
        for pair in range(PAIRS):
            some = heads[pair * per_group // PAIRS:(pair + 1) * per_group // PAIRS]

            def part_of_list(n):
                k = keys_of(n, FAR_CHUNK)
                v = blocks(1, n, FAR_CHUNK)
                scores = [jnp.dot(k, qt[i, g], preferred_element_type=jnp.float32) for g in some]
                old = [(total[i, g], acc[i, g]) for g in some]
                new = []
                for s, (amount, mix) in zip(scores, old):
                    p = jnp.exp2(s * SCALE)
                    amount = amount + jnp.sum(p, axis=0, keepdims=True)
                    mix = mix + lax.dot_general(v, p.astype(jnp.bfloat16), (((0,), (0,)), ((), ())),
                                                preferred_element_type=jnp.float32)
                    new.append((amount, mix))
                for g, (amount, mix) in zip(some, new):
                    total[i, g] = amount
                    acc[i, g] = mix

            def chunk(n, _):
                for j in range(FAR_PARTS):
                    part_of_list(n * FAR_PARTS + j)
                return 0

            lax.fori_loop(0, steps(FAR_CHUNK * FAR_PARTS), chunk, 0)
            for g in some:
                a = acc[i, g] * (1.0 / total[i, g])
                o_buf[i, :, g * HEAD_DIM:(g + 1) * HEAD_DIM] = a.T.astype(jnp.bfloat16)

            @pl.when(step < SIDE - 1)
            def _():
                o_copies(i, pair).start()

        return 0

    lax.fori_loop(0, SIDE, far_slab, 0)
    attn[c] = o_buf[c]
    for d in range(1, SIDE):
        for pair in range(PAIRS):
            there = attn.at[peer(d), :, pl.ds(pair * width // PAIRS, width // PAIRS)]
            remote(there, there, o_send.at[peer(d), pair], o_recv.at[peer(d), pair], next_plane).wait_recv()

    weight_copy.wait()
    tiles = give.shape[0]
    mine = pl.ds(pl.multiple_of(core * half, half), half)
    theirs = pl.ds(pl.multiple_of(other * half, half), half)

    def swap(t):
        return pltpu.make_async_remote_copy(
            src_ref=give.at[t], dst_ref=take.at[t], send_sem=x_send.at[t], recv_sem=x_recv.at[t],
            device_id=(me, other), device_id_type=MESH,
        )

    def project(t, _):
        columns = pl.ds(pl.multiple_of(t * tile, tile), tile)
        a = jnp.concatenate([attn[j] for j in range(SIDE)], axis=1)
        res[t] = jnp.dot(a, w_ref[:, columns], preferred_element_type=jnp.float32)
        give[t] = res[t, theirs, :].astype(jnp.bfloat16)
        swap(t).start()
        return 0

    lax.fori_loop(0, tiles, project, 0)

    def put(t):
        columns = pl.ds(pl.multiple_of(t * tile, tile), tile)
        return pltpu.make_async_copy(out_buf.at[:, columns], out_ref.at[:, columns], out_sem.at[t])

    def add_up(t, _):
        columns = pl.ds(pl.multiple_of(t * tile, tile), tile)
        swap(t).wait_recv()
        out_buf[:, columns] = (res[t, mine, :] + take[t].astype(jnp.float32)).astype(out_ref.dtype)
        put(t).start()
        return 0

    lax.fori_loop(0, tiles, add_up, 0)

    def swapped(t, _):
        swap(t).wait_send()
        return 0

    lax.fori_loop(0, tiles, swapped, 0)
    for d in range(1, SIDE):
        for part in range(2):
            pack_copy(part, d).wait_send()
        for copy in kv_copies(d):
            copy.wait_send()
        q_copy(d).wait_send()
        for pair in range(PAIRS):
            o_copies(peer(d), pair).wait_send()
    for copy in next_copies():
        copy.wait_send()
    for part in range(2):
        every = slots[part].at[pl.ds(0, (SIDE ** 3 - SIDE) * CAP)]
        remote(every, every, ring_send.at[part], slot_recv.at[part, 0], next_plane).wait_send()

    def stored(t, _):
        put(t).wait()
        return 0

    lax.fori_loop(0, tiles, stored, 0)


def on_device(n, queries, keys, values, vertical, slash, out_weight):
    rows = queries.shape[0]
    kv = vertical.shape[0]
    per_group = queries.shape[1] // (kv * HEAD_DIM)
    width = per_group * HEAD_DIM
    model = out_weight.shape[1]
    listed = vertical.shape[1]

    tile = math.gcd(model, 1024)
    tiles = model // tile
    vmem = pl.BlockSpec(memory_space=pltpu.VMEM)
    smem = pl.BlockSpec(memory_space=pltpu.SMEM)
    dma = pltpu.SemaphoreType.DMA
    return pl.pallas_call(
        functools.partial(kernel, per_group, tile),
        out_shape=jax.ShapeDtypeStruct((rows // 2, model), jnp.bfloat16),
        in_specs=[vmem] * 4 + [smem] * 2 + [pl.BlockSpec(memory_space=pl.ANY)],
        out_specs=pl.BlockSpec(memory_space=pl.ANY),
        scratch_shapes=[
            [pltpu.VMEM((kv, CAP, BLK, HEAD_DIM), jnp.bfloat16) for _ in range(2)],
            [pltpu.VMEM((n * CAP, BLK, HEAD_DIM), jnp.bfloat16) for _ in range(2)],
            pltpu.VMEM((SIDE, rows, width), jnp.bfloat16),
            pltpu.VMEM((SIDE, per_group, 2 * HEAD_DIM, rows), jnp.bfloat16),
            pltpu.VMEM((SIDE + 1, rows, HEAD_DIM), jnp.bfloat16),
            pltpu.VMEM((SIDE + 1, rows, HEAD_DIM), jnp.bfloat16),
            pltpu.VMEM((listed * BLK, HEAD_DIM), jnp.bfloat16),
            pltpu.SMEM((listed,), jnp.int32),
            pltpu.VMEM(out_weight.shape, jnp.bfloat16),
            pltpu.VMEM((SIDE, per_group, HEAD_DIM, rows), jnp.float32),
            pltpu.VMEM((SIDE, per_group, 1, rows), jnp.float32),
            pltpu.VMEM((SIDE, per_group, 1, rows), jnp.float32),
            pltpu.VMEM((SIDE, per_group, 1, rows), jnp.float32),
            pltpu.VMEM((SIDE, rows, width), jnp.bfloat16),
            pltpu.VMEM((SIDE, rows, width), jnp.bfloat16),
            pltpu.VMEM((tiles, rows, tile), jnp.float32),
            pltpu.VMEM((tiles, rows // 2, tile), jnp.bfloat16),
            pltpu.VMEM((tiles, rows // 2, tile), jnp.bfloat16),
            pltpu.VMEM((rows // 2, model), jnp.bfloat16),
            dma,
            dma((2, SIDE)),
            dma((SIDE, 2)),
            dma((SIDE + 1, 2)),
            dma((SIDE,)),
            dma((SIDE,)),
            dma((2, n)),
            dma((2,)),
            dma((SIDE, PAIRS)),
            dma((SIDE, PAIRS)),
            dma((tiles,)),
            dma((tiles,)),
            dma((tiles,)),
        ],
        compiler_params=pltpu.CompilerParams(
            collective_id=0, has_side_effects=True, vmem_limit_bytes=60 * 2**20
        ),
    )(queries, keys, values, vertical, vertical, slash.T, out_weight)


def solution(mesh):
    placed = (
        P("seq", "head"),
        P("seq", "head"),
        P("seq", "head"),
        P("head", None),
        P("head", None),
        P("head", None),
    )
    return jax.shard_map(
        functools.partial(on_device, mesh.shape["seq"]),
        mesh=mesh, in_specs=placed, out_specs=P(("seq", "head"), None), check_vma=False,
    )
```

```python
import functools
import math

import jax
import jax.numpy as jnp
from jax import lax
from jax.experimental import pallas as pl
from jax.experimental.pallas import tpu as pltpu
from jax.sharding import PartitionSpec as P

HEAD_DIM = 128
BLK = 64
CAP = 2
NEGATIVE = -1e30
MESH = pl.DeviceIdType.MESH
SCALE = HEAD_DIM ** (-0.5) * math.log2(math.e)
SIDE = 4
FAR_CHUNK = 32
PAIRS = 2
FAR_PARTS = 2
ENDS = 2 * SIDE * SIDE
TOP_CHUNK = 32
AUX = 16


def kernel(
    per_group, tile,
    q_hbm, k_hbm, v_hbm, vert_hbm, slash_hbm, w_hbm, out_ref,
    q_ref, k_ref, v_ref, list_ref, vert_ref, slash_ref,
    packs, slots, qg, qt, kg, vg, aux_k, places, w_ref, acc, top, far_top, total, o_buf, attn, give, take, out_buf,
    in_sem, w_sem, pack_send, kv_send, kv_recv, q_send, q_recv, slot_recv, ring_send,
    o_send, o_recv, x_send, x_recv, out_sem,
):
    rows = q_ref.shape[0]
    me = lax.axis_index("seq")
    core = lax.axis_index("head")
    other = 1 - core
    o, c = me // SIDE, me % SIDE
    x, z = o // SIDE, o % SIDE
    slab_blocks = rows // BLK
    half = rows // 2
    width = per_group * HEAD_DIM
    chosen_count = vert_ref.shape[1]
    next_plane = (me + SIDE) % (SIDE ** 3)
    last_plane = (me + SIDE ** 3 - SIDE) % (SIDE ** 3)

    def at(xx, zz, cc):
        return (xx % SIDE * SIDE + zz % SIDE) * SIDE + cc

    given = [
        pltpu.make_async_copy(source, here, in_sem.at[i])
        for i, (source, here) in enumerate((
            (vert_hbm, list_ref), (k_hbm, k_ref), (v_hbm, v_ref), (q_hbm, q_ref), (vert_hbm, vert_ref),
            (slash_hbm, slash_ref)))
    ]
    for copy in given:
        copy.start()

    barrier = pltpu.get_barrier_semaphore()

    def greet(seq, head):
        pl.semaphore_signal(barrier, inc=1, device_id=(seq, head), device_id_type=MESH)

    greet(me, other)
    for d in range(1, SIDE):
        greet(o * SIDE + (c + d) % SIDE, core)
    for step in range(1, SIDE):
        greet(at(x + step, z, c), core)
        greet(at(x, z + step, c), core)
    greet(next_plane, core)
    greet(last_plane, core)

    weight_copy = pltpu.make_async_copy(w_hbm, w_ref, w_sem)
    weight_copy.start()

    def lanes(h, size=HEAD_DIM):
        return pl.ds(pl.multiple_of(h * size, size), size)

    first_block = me * slab_blocks
    for copy in given:
        copy.wait()
    found = list_ref[...] - first_block
    inside = (found >= 0) & (found < slab_blocks)
    low = jnp.min(jnp.where(inside, found, slab_blocks), axis=1, keepdims=True)
    high = jnp.max(jnp.where(inside, found, -1), axis=1, keepdims=True)
    for h in range(SIDE):
        for slot, extreme in enumerate((low, high)):
            pick = jnp.broadcast_to(extreme[h:h + 1], (BLK, HEAD_DIM))
            for part, source in enumerate((k_ref, v_ref)):
                got = source[:BLK, h * HEAD_DIM:(h + 1) * HEAD_DIM]
                for i in range(1, slab_blocks):
                    rows_i = source[i * BLK:(i + 1) * BLK, h * HEAD_DIM:(h + 1) * HEAD_DIM]
                    got = jnp.where(pick == i, rows_i, got)
                packs[part][h, slot] = got
    for part in range(2):
        for i in range(CAP):
            slots[part][me * CAP + i] = packs[part][c, i]
    kg[c + 1] = k_ref[:, lanes(c)]
    vg[c + 1] = v_ref[:, lanes(c)]
    qg[c] = q_ref[:, lanes(c, width)]

    pl.semaphore_wait(barrier, 1 + 3 * (SIDE - 1) + 2)

    def remote(src, dst, send_sem, recv_sem, seq):
        return pltpu.make_async_remote_copy(
            src_ref=src, dst_ref=dst, send_sem=send_sem, recv_sem=recv_sem,
            device_id=(seq, core), device_id_type=MESH,
        )

    def held(part, slab):
        return slots[part].at[pl.ds(slab * CAP, CAP)]

    def peer(d):
        return (c + d) % SIDE

    def pack_copy(part, d):
        return remote(packs[part].at[peer(d)], held(part, me), pack_send.at[part, d], slot_recv.at[part, c],
                      o * SIDE + peer(d))

    def kv_copies(d):
        to = peer(d)
        return [
            remote(source.at[:, lanes(to)], got.at[c + 1], kv_send.at[d, i], kv_recv.at[c + 1, i], o * SIDE + to)
            for i, (source, got) in enumerate(((k_ref, kg), (v_ref, vg)))
        ]

    def q_copy(d):
        to = peer(d)
        return remote(q_ref.at[:, lanes(to, width)], qg.at[c], q_send.at[d], q_recv.at[c], o * SIDE + to)

    def next_copies():
        return [
            remote(got.at[SIDE], got.at[0], kv_send.at[0, i], kv_recv.at[0, i], next_plane)
            for i, got in enumerate((kg, vg))
        ]

    near_order = (1, SIDE - 1, 2)
    for d in near_order:
        pack_copy(0, d).start()

    def slab_of(dp, dq, kind):
        x_first = kind < 2
        return jnp.where(x_first, at(x + SIDE - dp, z + SIDE - dq, kind), at(x + SIDE - dq, z + SIDE - dp, kind))

    def ring(part, slab, kind, phase, sign, mark):
        x_first = kind < 2
        along_x = x_first if phase == 0 else jnp.logical_not(x_first)
        to = jnp.where(along_x, at(x + SIDE + sign, z, c), at(x, z + SIDE + sign, c))
        there = held(part, slab)
        return remote(there, there, ring_send.at[part], slot_recv.at[part, mark], to)

    def in_group(kind):
        return kind

    def in_first(dp, kind):
        return SIDE + (dp % SIDE - 1) * SIDE + kind

    def in_second(dp, sign, kind):
        return jnp.where(kind % 2 == (1 - sign) // 2, SIDE * (SIDE + dp % SIDE) + kind, ENDS)

    def arrived(part, slab, mark):
        there = held(part, slab)
        remote(there, there, pack_send.at[part, 1], slot_recv.at[part, mark], next_plane).wait_recv()

    def first(part, ds=(0, SIDE - 1, 1, 2)):
        for d in ds:
            kind = peer(d)
            for dp in (1, -1, 2):
                slab = slab_of(dp, 0, kind)
                arrived(part, slab, in_first(dp, kind))
                for sign in (1, -1):
                    ring(part, slab, kind, 1, sign, in_second(dp, sign, kind)).start()

    def second(part, dp):
        for kind in range(SIDE):
            sign = 1 if kind % 2 == 0 else -1
            slab = slab_of(dp, sign, kind)
            arrived(part, slab, in_second(dp, sign, kind))
            ring(part, slab, kind, 1, sign, ENDS).start()

    def pass_own(part, ds):
        for d in ds:
            slab = o * SIDE + peer(d)
            kind = peer(d)
            if d:
                arrived(part, slab, in_group(kind))
            for step in (1, -1, 2):
                ring(part, slab, kind, 0, step, in_first(step, kind)).start()
            for sign in (1, -1):
                ring(part, slab, kind, 1, sign, in_second(0, sign, kind)).start()

    pass_own(0, (0,))
    lane = lax.broadcasted_iota(jnp.int32, (BLK, HEAD_DIM), 1)
    limit = (o * SIDE + lane - 1) * slab_blocks
    unit = jnp.where((lane >= SIDE) & (lane < SIDE + 3), 1.0, 0.0)

    def look_up(n, _):
        for j in range(8):
            e = n * 8 + j
            block = vert_ref[c, e]
            slab = block // slab_blocks
            before = jnp.where(e > 0, vert_ref[c, jnp.maximum(e - 1, 0)] // slab_blocks, -1)
            places[e] = slab * CAP + jnp.where(before == slab, 1, 0)
            mask = jnp.where((lane < SIDE) & (block >= limit), NEGATIVE, unit)
            aux_k[pl.ds(pl.multiple_of(e * BLK, BLK), BLK), :] = mask.astype(jnp.bfloat16)
        return 0

    lax.fori_loop(0, chosen_count // 8, look_up, 0)
    pass_own(0, (SIDE - 1, 1, 2))
    for d in near_order:
        for copy in kv_copies(d):
            copy.start()
    for d in near_order:
        pack_copy(1, d).start()
    for d in (SIDE - 1, 1, 2):
        q_copy(d).start()
    first(0)

    heads = range(per_group)

    def turn(i):
        row = lax.broadcasted_iota(jnp.int32, (HEAD_DIM, rows), 0)
        for g in heads:
            qt[i, g, :HEAD_DIM] = qg[i, :, g * HEAD_DIM:(g + 1) * HEAD_DIM].T
            qt[i, g, HEAD_DIM:] = jnp.where(row == i, 1.0, 0.0).astype(jnp.bfloat16)

    def near(i):
        base = (o * SIDE + i) * slab_blocks
        k = jnp.concatenate([kg[i], kg[i + 1]], axis=0)
        vt = jnp.concatenate([vg[i], vg[i + 1]], axis=0).T
        shape = (2 * slab_blocks, rows)
        block = lax.broadcasted_iota(jnp.int32, shape, 0) - slab_blocks
        gap = lax.broadcasted_iota(jnp.int32, shape, 1) // BLK - block
        block = base + block
        good = gap == 0
        for j in range(slash_ref.shape[0]):
            good = good | (gap == slash_ref[j, c])
        chosen = block == vert_ref[c, 0]
        for e in range(1, chosen_count):
            chosen = chosen | (block == vert_ref[c, e])
        good = good | (chosen & (gap > 0))
        bias = jnp.where(good & (block >= 0), 0.0, NEGATIVE)
        keys_at = lax.broadcasted_iota(jnp.int32, (rows, rows), 0)
        query_at = lax.broadcasted_iota(jnp.int32, (rows, rows), 1)
        causal = keys_at <= query_at
        scores = []
        for g in heads:
            scores.append(jnp.dot(k, qt[i, g, :HEAD_DIM], preferred_element_type=jnp.float32))
        for g, s in zip(heads, scores):
            s = jnp.concatenate(
                [s[j * BLK:(j + 1) * BLK] + bias[j:j + 1] for j in range(2 * slab_blocks)], axis=0)
            s = jnp.concatenate([s[:rows], jnp.where(causal, s[rows:], NEGATIVE)], axis=0)
            peak = jnp.max(s, axis=0, keepdims=True)
            p = jnp.exp2((s - peak) * SCALE)
            top[i, g] = peak
            total[i, g] = jnp.sum(p, axis=0, keepdims=True)
            acc[i, g] = jnp.dot(vt, p.astype(jnp.bfloat16), preferred_element_type=jnp.float32)

    def second_keys(dp, _):
        second(0, dp)
        return 0

    def last_ones(part):
        every = slots[part].at[pl.ds(0, 2 * SIDE * SIDE * CAP)]
        remote(every, every, pack_send.at[part, 1], slot_recv.at[part, ENDS], next_plane).wait_recv()

    lax.fori_loop(0, SIDE, second_keys, 0)
    pass_own(1, (0, SIDE - 1, 1, 2))
    for d in range(1, SIDE):
        for i, got in enumerate((kg, vg)):
            there = got.at[peer(d) + 1]
            remote(there, there, kv_send.at[d, i], kv_recv.at[peer(d) + 1, i], next_plane).wait_recv()
    for copy in next_copies():
        copy.start()

    def queries_in(i):
        remote(qg.at[i], qg.at[i], q_send.at[1], q_recv.at[i], next_plane).wait_recv()

    turn(c)

    @pl.when(c > 0)
    def _():
        near(c)

    last_ones(0)

    def blocks(part, n, size):
        return jnp.concatenate([slots[part][places[n * size + j]] for j in range(size)], axis=0)

    def keys_of(n, size):
        masks = aux_k[pl.ds(pl.multiple_of(n * size * BLK, size * BLK), size * BLK), :]
        return jnp.concatenate([blocks(0, n, size), masks], axis=1)

    def steps(size):
        return jnp.minimum(chosen_count, (o * SIDE + 2) * CAP + size - 1) // size

    def largest(i):
        def chunk(n, peaks):
            k = keys_of(n, TOP_CHUNK)
            return tuple(
                jnp.maximum(peak, jnp.max(jnp.dot(k, qt[i, g], preferred_element_type=jnp.float32),
                                          axis=0, keepdims=True))
                for g, peak in zip(heads, peaks))

        peaks = lax.fori_loop(0, steps(TOP_CHUNK), chunk, (jnp.full((1, rows), NEGATIVE),) * per_group)
        for g, peak in zip(heads, peaks):
            far_top[i, g] = peak

    def join(i):
        row = lax.broadcasted_iota(jnp.int32, (AUX, rows), 0)
        for g in heads:
            old = top[i, g]
            peak = jnp.maximum(old, far_top[i, g])
            shrink = jnp.exp2((old - peak) * SCALE)
            total[i, g] = total[i, g] * shrink
            acc[i, g] = acc[i, g] * shrink
            rest = -peak
            aux = jnp.where(row == i, 1.0, 0.0)
            for j in range(3):
                part = rest.astype(jnp.bfloat16).astype(jnp.float32)
                aux = jnp.where(row == SIDE + j, part, aux)
                rest = rest - part
            qt[i, g, HEAD_DIM:HEAD_DIM + AUX] = aux.astype(jnp.bfloat16)

    def first_pass(step, _):
        i = (c + step + jnp.where(step == 2, 1, jnp.where(step == 3, -1, 0))) % SIDE

        @pl.when(step > 0)
        def _():
            queries_in(i)
            turn(i)

        largest(i)

        @pl.when(step == 0)
        def _():
            first(1, (0, SIDE - 1))

        @pl.when(step == 1)
        def _():
            first(1, (1, 2))

        def values_second(j, _):
            second(1, (2 + j) % SIDE)
            return 0

        lax.fori_loop(jnp.where(step == 2, 1, jnp.where(step == 3, 0, SIDE)),
                      jnp.where(step == 3, 1, SIDE), values_second, 0)
        return 0

    lax.fori_loop(0, SIDE, first_pass, 0)
    for copy in next_copies():
        copy.wait_recv()

    def other_near(i, _):
        @pl.when(i != c)
        def _():
            near(i)

        return 0

    lax.fori_loop(0, SIDE, other_near, 0)
    last_ones(1)

    def o_copies(i, pair):
        columns = pl.ds(pair * width // PAIRS, width // PAIRS)
        return remote(o_buf.at[i, :, columns], attn.at[c, :, columns], o_send.at[i, pair], o_recv.at[c, pair], o * SIDE + i)

    def far_slab(step, _):
        i = (c + SIDE - 1 - step) % SIDE

        @pl.when((step == SIDE - 1) & (c == 0))
        def _():
            near(i)

        join(i)
        for pair in range(PAIRS):
            some = heads[pair * per_group // PAIRS:(pair + 1) * per_group // PAIRS]

            def part_of_list(n):
                k = keys_of(n, FAR_CHUNK)
                v = blocks(1, n, FAR_CHUNK)
                scores = [jnp.dot(k, qt[i, g], preferred_element_type=jnp.float32) for g in some]
                old = [(total[i, g], acc[i, g]) for g in some]
                new = []
                for s, (amount, mix) in zip(scores, old):
                    p = jnp.exp2(s * SCALE)
                    amount = amount + jnp.sum(p, axis=0, keepdims=True)
                    mix = mix + lax.dot_general(v, p.astype(jnp.bfloat16), (((0,), (0,)), ((), ())),
                                                preferred_element_type=jnp.float32)
                    new.append((amount, mix))
                for g, (amount, mix) in zip(some, new):
                    total[i, g] = amount
                    acc[i, g] = mix

            def chunk(n, _):
                for j in range(FAR_PARTS):
                    part_of_list(n * FAR_PARTS + j)
                return 0

            lax.fori_loop(0, steps(FAR_CHUNK * FAR_PARTS), chunk, 0)
            for g in some:
                a = acc[i, g] * (1.0 / total[i, g])
                o_buf[i, :, g * HEAD_DIM:(g + 1) * HEAD_DIM] = a.T.astype(jnp.bfloat16)

            @pl.when(step < SIDE - 1)
            def _():
                o_copies(i, pair).start()

        return 0

    lax.fori_loop(0, SIDE, far_slab, 0)
    attn[c] = o_buf[c]
    for d in range(1, SIDE):
        for pair in range(PAIRS):
            there = attn.at[peer(d), :, pl.ds(pair * width // PAIRS, width // PAIRS)]
            remote(there, there, o_send.at[peer(d), pair], o_recv.at[peer(d), pair], next_plane).wait_recv()

    weight_copy.wait()
    tiles = give.shape[0]
    mine = pl.ds(pl.multiple_of(core * half, half), half)
    theirs = pl.ds(pl.multiple_of(other * half, half), half)

    def swap(t):
        return pltpu.make_async_remote_copy(
            src_ref=give.at[t], dst_ref=take.at[t], send_sem=x_send.at[t], recv_sem=x_recv.at[t],
            device_id=(me, other), device_id_type=MESH,
        )

    def project(t, place):
        columns = pl.ds(pl.multiple_of(t * tile, tile), tile)
        a = jnp.concatenate([attn[j, place, :] for j in range(SIDE)], axis=1)
        return jnp.dot(a, w_ref[:, columns], preferred_element_type=jnp.float32)

    def share(t, _):
        give[t] = project(t, theirs).astype(jnp.bfloat16)
        swap(t).start()
        return 0

    lax.fori_loop(0, tiles, share, 0)

    def put(t):
        columns = pl.ds(pl.multiple_of(t * tile, tile), tile)
        return pltpu.make_async_copy(out_buf.at[:, columns], out_ref.at[:, columns], out_sem.at[t])

    def add_up(t, _):
        columns = pl.ds(pl.multiple_of(t * tile, tile), tile)
        swap(t).wait_recv()
        out_buf[:, columns] = (project(t, mine) + take[t].astype(jnp.float32)).astype(out_ref.dtype)
        put(t).start()
        return 0

    lax.fori_loop(0, tiles, add_up, 0)

    def swapped(t, _):
        swap(t).wait_send()
        return 0

    lax.fori_loop(0, tiles, swapped, 0)
    for d in range(1, SIDE):
        for part in range(2):
            pack_copy(part, d).wait_send()
        for copy in kv_copies(d):
            copy.wait_send()
        q_copy(d).wait_send()
        for pair in range(PAIRS):
            o_copies(peer(d), pair).wait_send()
    for copy in next_copies():
        copy.wait_send()
    for part in range(2):
        every = slots[part].at[pl.ds(0, (SIDE ** 3 - SIDE) * CAP)]
        remote(every, every, ring_send.at[part], slot_recv.at[part, 0], next_plane).wait_send()

    def stored(t, _):
        put(t).wait()
        return 0

    lax.fori_loop(0, tiles, stored, 0)


def on_device(n, queries, keys, values, vertical, slash, out_weight):
    rows = queries.shape[0]
    kv = vertical.shape[0]
    per_group = queries.shape[1] // (kv * HEAD_DIM)
    width = per_group * HEAD_DIM
    model = out_weight.shape[1]
    listed = vertical.shape[1]

    tile = math.gcd(model, 1024)
    tiles = model // tile
    dma = pltpu.SemaphoreType.DMA
    return pl.pallas_call(
        functools.partial(kernel, per_group, tile),
        out_shape=jax.ShapeDtypeStruct((rows // 2, model), jnp.bfloat16),
        in_specs=[pl.BlockSpec(memory_space=pl.ANY)] * 6,
        out_specs=pl.BlockSpec(memory_space=pl.ANY),
        scratch_shapes=[
            pltpu.VMEM(queries.shape, jnp.bfloat16),
            pltpu.VMEM(keys.shape, jnp.bfloat16),
            pltpu.VMEM(values.shape, jnp.bfloat16),
            pltpu.VMEM(vertical.shape, jnp.int32),
            pltpu.SMEM(vertical.shape, jnp.int32),
            pltpu.SMEM(slash.T.shape, jnp.int32),
            [pltpu.VMEM((kv, CAP, BLK, HEAD_DIM), jnp.bfloat16) for _ in range(2)],
            [pltpu.VMEM((n * CAP, BLK, HEAD_DIM), jnp.bfloat16) for _ in range(2)],
            pltpu.VMEM((SIDE, rows, width), jnp.bfloat16),
            pltpu.VMEM((SIDE, per_group, 2 * HEAD_DIM, rows), jnp.bfloat16),
            pltpu.VMEM((SIDE + 1, rows, HEAD_DIM), jnp.bfloat16),
            pltpu.VMEM((SIDE + 1, rows, HEAD_DIM), jnp.bfloat16),
            pltpu.VMEM((listed * BLK, HEAD_DIM), jnp.bfloat16),
            pltpu.SMEM((listed,), jnp.int32),
            pltpu.VMEM(out_weight.shape, jnp.bfloat16),
            pltpu.VMEM((SIDE, per_group, HEAD_DIM, rows), jnp.float32),
            pltpu.VMEM((SIDE, per_group, 1, rows), jnp.float32),
            pltpu.VMEM((SIDE, per_group, 1, rows), jnp.float32),
            pltpu.VMEM((SIDE, per_group, 1, rows), jnp.float32),
            pltpu.VMEM((SIDE, rows, width), jnp.bfloat16),
            pltpu.VMEM((SIDE, rows, width), jnp.bfloat16),
            pltpu.VMEM((tiles, rows // 2, tile), jnp.bfloat16),
            pltpu.VMEM((tiles, rows // 2, tile), jnp.bfloat16),
            pltpu.VMEM((rows // 2, model), jnp.bfloat16),
            dma((6,)),
            dma,
            dma((2, SIDE)),
            dma((SIDE, 2)),
            dma((SIDE + 1, 2)),
            dma((SIDE,)),
            dma((SIDE,)),
            dma((2, ENDS + 1)),
            dma((2,)),
            dma((SIDE, PAIRS)),
            dma((SIDE, PAIRS)),
            dma((tiles,)),
            dma((tiles,)),
            dma((tiles,)),
        ],
        compiler_params=pltpu.CompilerParams(
            collective_id=0, has_side_effects=True, vmem_limit_bytes=60 * 2**20
        ),
    )(queries, keys, values, vertical, slash.T, out_weight)


def solution(mesh):
    placed = (
        P("seq", "head"),
        P("seq", "head"),
        P("seq", "head"),
        P("head", None),
        P("head", None),
        P("head", None),
    )
    return jax.shard_map(
        functools.partial(on_device, mesh.shape["seq"]),
        mesh=mesh, in_specs=placed, out_specs=P(("seq", "head"), None), check_vma=False,
    )
```

```python
import functools
import math

import jax
import jax.numpy as jnp
from jax import lax
from jax.experimental import pallas as pl
from jax.experimental.pallas import tpu as pltpu
from jax.sharding import PartitionSpec as P

HEAD_DIM = 128
BLK = 64
CAP = 2
NEGATIVE = -1e30
MESH = pl.DeviceIdType.MESH
SCALE = HEAD_DIM ** (-0.5) * math.log2(math.e)
SIDE = 4
FAR_CHUNK = 32
PAIRS = 2
FAR_PARTS = 2
ENDS = 2 * SIDE * SIDE
EARLY = 2
TOP_CHUNK = 32
AUX = 16


def kernel(
    per_group, tile,
    q_hbm, k_hbm, v_hbm, vert_hbm, slash_hbm, w_hbm, out_ref,
    q_ref, k_ref, v_ref, list_ref, vert_ref, slash_ref,
    packs, slots, qg, qt, kg, vg, aux_k, places, w_ref, acc, top, far_top, total, o_buf, attn, early, give, take, out_buf,
    in_sem, w_sem, pack_send, kv_send, kv_recv, q_send, q_recv, slot_recv, ring_send,
    o_send, o_recv, x_send, x_recv, out_sem,
):
    rows = q_ref.shape[0]
    me = lax.axis_index("seq")
    core = lax.axis_index("head")
    other = 1 - core
    o, c = me // SIDE, me % SIDE
    x, z = o // SIDE, o % SIDE
    slab_blocks = rows // BLK
    half = rows // 2
    width = per_group * HEAD_DIM
    chosen_count = vert_ref.shape[1]
    next_plane = (me + SIDE) % (SIDE ** 3)
    last_plane = (me + SIDE ** 3 - SIDE) % (SIDE ** 3)

    def at(xx, zz, cc):
        return (xx % SIDE * SIDE + zz % SIDE) * SIDE + cc

    given = [
        pltpu.make_async_copy(source, here, in_sem.at[i])
        for i, (source, here) in enumerate((
            (vert_hbm, list_ref), (k_hbm, k_ref), (v_hbm, v_ref), (q_hbm, q_ref), (vert_hbm, vert_ref),
            (slash_hbm, slash_ref)))
    ]
    for copy in given:
        copy.start()

    barrier = pltpu.get_barrier_semaphore()

    def greet(seq, head):
        pl.semaphore_signal(barrier, inc=1, device_id=(seq, head), device_id_type=MESH)

    greet(me, other)
    for d in range(1, SIDE):
        greet(o * SIDE + (c + d) % SIDE, core)
    for step in range(1, SIDE):
        greet(at(x + step, z, c), core)
        greet(at(x, z + step, c), core)
    greet(next_plane, core)
    greet(last_plane, core)

    weight_copy = pltpu.make_async_copy(w_hbm, w_ref, w_sem)
    weight_copy.start()

    def lanes(h, size=HEAD_DIM):
        return pl.ds(pl.multiple_of(h * size, size), size)

    first_block = me * slab_blocks
    for copy in given:
        copy.wait()
    found = list_ref[...] - first_block
    inside = (found >= 0) & (found < slab_blocks)
    low = jnp.min(jnp.where(inside, found, slab_blocks), axis=1, keepdims=True)
    high = jnp.max(jnp.where(inside, found, -1), axis=1, keepdims=True)
    for h in range(SIDE):
        for slot, extreme in enumerate((low, high)):
            pick = jnp.broadcast_to(extreme[h:h + 1], (BLK, HEAD_DIM))
            for part, source in enumerate((k_ref, v_ref)):
                got = source[:BLK, h * HEAD_DIM:(h + 1) * HEAD_DIM]
                for i in range(1, slab_blocks):
                    rows_i = source[i * BLK:(i + 1) * BLK, h * HEAD_DIM:(h + 1) * HEAD_DIM]
                    got = jnp.where(pick == i, rows_i, got)
                packs[part][h, slot] = got
    for part in range(2):
        for i in range(CAP):
            slots[part][me * CAP + i] = packs[part][c, i]
    kg[c + 1] = k_ref[:, lanes(c)]
    vg[c + 1] = v_ref[:, lanes(c)]
    qg[c] = q_ref[:, lanes(c, width)]

    pl.semaphore_wait(barrier, 1 + 3 * (SIDE - 1) + 2)

    def remote(src, dst, send_sem, recv_sem, seq):
        return pltpu.make_async_remote_copy(
            src_ref=src, dst_ref=dst, send_sem=send_sem, recv_sem=recv_sem,
            device_id=(seq, core), device_id_type=MESH,
        )

    def held(part, slab):
        return slots[part].at[pl.ds(slab * CAP, CAP)]

    def peer(d):
        return (c + d) % SIDE

    def pack_copy(part, d):
        return remote(packs[part].at[peer(d)], held(part, me), pack_send.at[part, d], slot_recv.at[part, c],
                      o * SIDE + peer(d))

    def kv_copies(d):
        to = peer(d)
        return [
            remote(source.at[:, lanes(to)], got.at[c + 1], kv_send.at[d, i], kv_recv.at[c + 1, i], o * SIDE + to)
            for i, (source, got) in enumerate(((k_ref, kg), (v_ref, vg)))
        ]

    def q_copy(d):
        to = peer(d)
        return remote(q_ref.at[:, lanes(to, width)], qg.at[c], q_send.at[d], q_recv.at[c], o * SIDE + to)

    def next_copies():
        return [
            remote(got.at[SIDE], got.at[0], kv_send.at[0, i], kv_recv.at[0, i], next_plane)
            for i, got in enumerate((kg, vg))
        ]

    near_order = (1, SIDE - 1, 2)
    for d in near_order:
        pack_copy(0, d).start()

    def slab_of(dp, dq, kind):
        x_first = kind < 2
        return jnp.where(x_first, at(x + SIDE - dp, z + SIDE - dq, kind), at(x + SIDE - dq, z + SIDE - dp, kind))

    def ring(part, slab, kind, phase, sign, mark):
        x_first = kind < 2
        along_x = x_first if phase == 0 else jnp.logical_not(x_first)
        to = jnp.where(along_x, at(x + SIDE + sign, z, c), at(x, z + SIDE + sign, c))
        there = held(part, slab)
        return remote(there, there, ring_send.at[part], slot_recv.at[part, mark], to)

    def in_group(kind):
        return kind

    def in_first(dp, kind):
        return SIDE + (dp % SIDE - 1) * SIDE + kind

    def in_second(dp, sign, kind):
        return jnp.where(kind % 2 == (1 - sign) // 2, SIDE * (SIDE + dp % SIDE) + kind, ENDS)

    def arrived(part, slab, mark):
        there = held(part, slab)
        remote(there, there, pack_send.at[part, 1], slot_recv.at[part, mark], next_plane).wait_recv()

    def first(part, ds=(0, SIDE - 1, 1, 2)):
        for d in ds:
            kind = peer(d)
            for dp in (1, -1, 2):
                slab = slab_of(dp, 0, kind)
                arrived(part, slab, in_first(dp, kind))
                for sign in (1, -1):
                    ring(part, slab, kind, 1, sign, in_second(dp, sign, kind)).start()

    def second(part, dp):
        for kind in range(SIDE):
            sign = 1 if kind % 2 == 0 else -1
            slab = slab_of(dp, sign, kind)
            arrived(part, slab, in_second(dp, sign, kind))
            ring(part, slab, kind, 1, sign, ENDS).start()

    def pass_own(part, ds):
        for d in ds:
            slab = o * SIDE + peer(d)
            kind = peer(d)
            if d:
                arrived(part, slab, in_group(kind))
            for step in (1, -1, 2):
                ring(part, slab, kind, 0, step, in_first(step, kind)).start()
            for sign in (1, -1):
                ring(part, slab, kind, 1, sign, in_second(0, sign, kind)).start()

    pass_own(0, (0,))
    lane = lax.broadcasted_iota(jnp.int32, (BLK, HEAD_DIM), 1)
    limit = (o * SIDE + lane - 1) * slab_blocks
    unit = jnp.where((lane >= SIDE) & (lane < SIDE + 3), 1.0, 0.0)

    def look_up(n, _):
        for j in range(8):
            e = n * 8 + j
            block = vert_ref[c, e]
            slab = block // slab_blocks
            before = jnp.where(e > 0, vert_ref[c, jnp.maximum(e - 1, 0)] // slab_blocks, -1)
            places[e] = slab * CAP + jnp.where(before == slab, 1, 0)
            mask = jnp.where((lane < SIDE) & (block >= limit), NEGATIVE, unit)
            aux_k[pl.ds(pl.multiple_of(e * BLK, BLK), BLK), :] = mask.astype(jnp.bfloat16)
        return 0

    lax.fori_loop(0, chosen_count // 8, look_up, 0)
    pass_own(0, (SIDE - 1, 1, 2))
    for d in near_order:
        for copy in kv_copies(d):
            copy.start()
    for d in near_order:
        pack_copy(1, d).start()
    for d in (SIDE - 1, 1, 2):
        q_copy(d).start()
    first(0)

    heads = range(per_group)

    def turn(i):
        row = lax.broadcasted_iota(jnp.int32, (HEAD_DIM, rows), 0)
        for g in heads:
            qt[i, g, :HEAD_DIM] = qg[i, :, g * HEAD_DIM:(g + 1) * HEAD_DIM].T
            qt[i, g, HEAD_DIM:] = jnp.where(row == i, 1.0, 0.0).astype(jnp.bfloat16)

    def near(i):
        base = (o * SIDE + i) * slab_blocks
        k = jnp.concatenate([kg[i], kg[i + 1]], axis=0)
        vt = jnp.concatenate([vg[i], vg[i + 1]], axis=0).T
        shape = (2 * slab_blocks, rows)
        block = lax.broadcasted_iota(jnp.int32, shape, 0) - slab_blocks
        gap = lax.broadcasted_iota(jnp.int32, shape, 1) // BLK - block
        block = base + block
        good = gap == 0
        for j in range(slash_ref.shape[0]):
            good = good | (gap == slash_ref[j, c])
        chosen = block == vert_ref[c, 0]
        for e in range(1, chosen_count):
            chosen = chosen | (block == vert_ref[c, e])
        good = good | (chosen & (gap > 0))
        bias = jnp.where(good & (block >= 0), 0.0, NEGATIVE)
        keys_at = lax.broadcasted_iota(jnp.int32, (rows, rows), 0)
        query_at = lax.broadcasted_iota(jnp.int32, (rows, rows), 1)
        causal = keys_at <= query_at
        scores = []
        for g in heads:
            scores.append(jnp.dot(k, qt[i, g, :HEAD_DIM], preferred_element_type=jnp.float32))
        for g, s in zip(heads, scores):
            s = jnp.concatenate(
                [s[j * BLK:(j + 1) * BLK] + bias[j:j + 1] for j in range(2 * slab_blocks)], axis=0)
            s = jnp.concatenate([s[:rows], jnp.where(causal, s[rows:], NEGATIVE)], axis=0)
            peak = jnp.max(s, axis=0, keepdims=True)
            p = jnp.exp2((s - peak) * SCALE)
            top[i, g] = peak
            total[i, g] = jnp.sum(p, axis=0, keepdims=True)
            acc[i, g] = jnp.dot(vt, p.astype(jnp.bfloat16), preferred_element_type=jnp.float32)

    def second_keys(dp, _):
        second(0, dp)
        return 0

    def last_ones(part):
        every = slots[part].at[pl.ds(0, 2 * SIDE * SIDE * CAP)]
        remote(every, every, pack_send.at[part, 1], slot_recv.at[part, ENDS], next_plane).wait_recv()

    lax.fori_loop(0, SIDE, second_keys, 0)
    pass_own(1, (0, SIDE - 1, 1, 2))
    for d in range(1, SIDE):
        for i, got in enumerate((kg, vg)):
            there = got.at[peer(d) + 1]
            remote(there, there, kv_send.at[d, i], kv_recv.at[peer(d) + 1, i], next_plane).wait_recv()
    for copy in next_copies():
        copy.start()

    def queries_in(i):
        remote(qg.at[i], qg.at[i], q_send.at[1], q_recv.at[i], next_plane).wait_recv()

    turn(c)

    @pl.when(c > 0)
    def _():
        near(c)

    last_ones(0)

    def blocks(part, n, size):
        return jnp.concatenate([slots[part][places[n * size + j]] for j in range(size)], axis=0)

    def keys_of(n, size):
        masks = aux_k[pl.ds(pl.multiple_of(n * size * BLK, size * BLK), size * BLK), :]
        return jnp.concatenate([blocks(0, n, size), masks], axis=1)

    def steps(size):
        return jnp.minimum(chosen_count, (o * SIDE + 2) * CAP + size - 1) // size

    def largest(i):
        def chunk(n, peaks):
            k = keys_of(n, TOP_CHUNK)
            return tuple(
                jnp.maximum(peak, jnp.max(jnp.dot(k, qt[i, g], preferred_element_type=jnp.float32),
                                          axis=0, keepdims=True))
                for g, peak in zip(heads, peaks))

        peaks = lax.fori_loop(0, steps(TOP_CHUNK), chunk, (jnp.full((1, rows), NEGATIVE),) * per_group)
        for g, peak in zip(heads, peaks):
            far_top[i, g] = peak

    def join(i):
        row = lax.broadcasted_iota(jnp.int32, (AUX, rows), 0)
        for g in heads:
            old = top[i, g]
            peak = jnp.maximum(old, far_top[i, g])
            shrink = jnp.exp2((old - peak) * SCALE)
            total[i, g] = total[i, g] * shrink
            acc[i, g] = acc[i, g] * shrink
            rest = -peak
            aux = jnp.where(row == i, 1.0, 0.0)
            for j in range(3):
                part = rest.astype(jnp.bfloat16).astype(jnp.float32)
                aux = jnp.where(row == SIDE + j, part, aux)
                rest = rest - part
            qt[i, g, HEAD_DIM:HEAD_DIM + AUX] = aux.astype(jnp.bfloat16)

    def first_pass(step, _):
        i = (c + step + jnp.where(step == 2, 1, jnp.where(step == 3, -1, 0))) % SIDE

        @pl.when(step > 0)
        def _():
            queries_in(i)
            turn(i)

        largest(i)

        @pl.when(step == 0)
        def _():
            first(1, (0, SIDE - 1))

        @pl.when(step == 1)
        def _():
            first(1, (1, 2))

        def values_second(j, _):
            second(1, (2 + j) % SIDE)
            return 0

        lax.fori_loop(jnp.where(step == 2, 1, jnp.where(step == 3, 0, SIDE)),
                      jnp.where(step == 3, 1, SIDE), values_second, 0)
        return 0

    lax.fori_loop(0, SIDE, first_pass, 0)
    for copy in next_copies():
        copy.wait_recv()

    def other_near(i, _):
        @pl.when(i != c)
        def _():
            near(i)

        return 0

    lax.fori_loop(0, SIDE, other_near, 0)
    last_ones(1)

    def o_copies(i, pair):
        columns = pl.ds(pair * width // PAIRS, width // PAIRS)
        return remote(o_buf.at[i, :, columns], attn.at[c, :, columns], o_send.at[i, pair], o_recv.at[c, pair], o * SIDE + i)

    def far_slab(step, _):
        i = (c + SIDE - 1 - step) % SIDE

        @pl.when((step == SIDE - 1) & (c == 0))
        def _():
            near(i)

        join(i)
        for pair in range(PAIRS):
            some = heads[pair * per_group // PAIRS:(pair + 1) * per_group // PAIRS]

            def part_of_list(n):
                k = keys_of(n, FAR_CHUNK)
                v = blocks(1, n, FAR_CHUNK)
                scores = [jnp.dot(k, qt[i, g], preferred_element_type=jnp.float32) for g in some]
                old = [(total[i, g], acc[i, g]) for g in some]
                new = []
                for s, (amount, mix) in zip(scores, old):
                    p = jnp.exp2(s * SCALE)
                    amount = amount + jnp.sum(p, axis=0, keepdims=True)
                    mix = mix + lax.dot_general(v, p.astype(jnp.bfloat16), (((0,), (0,)), ((), ())),
                                                preferred_element_type=jnp.float32)
                    new.append((amount, mix))
                for g, (amount, mix) in zip(some, new):
                    total[i, g] = amount
                    acc[i, g] = mix

            def chunk(n, _):
                for j in range(FAR_PARTS):
                    part_of_list(n * FAR_PARTS + j)
                return 0

            lax.fori_loop(0, steps(FAR_CHUNK * FAR_PARTS), chunk, 0)
            for g in some:
                a = acc[i, g] * (1.0 / total[i, g])
                o_buf[i, :, g * HEAD_DIM:(g + 1) * HEAD_DIM] = a.T.astype(jnp.bfloat16)

            @pl.when(step < SIDE - 1)
            def _():
                o_copies(i, pair).start()

        return 0

    lax.fori_loop(0, SIDE, far_slab, 0)
    attn[c] = o_buf[c]

    def heads_in(d):
        for pair in range(PAIRS):
            there = attn.at[peer(d), :, pl.ds(pair * width // PAIRS, width // PAIRS)]
            remote(there, there, o_send.at[peer(d), pair], o_recv.at[peer(d), pair], next_plane).wait_recv()

    for d in range(1, SIDE - 1):
        heads_in(d)

    weight_copy.wait()
    tiles = give.shape[0]
    mine = pl.ds(pl.multiple_of(core * half, half), half)
    theirs = pl.ds(pl.multiple_of(other * half, half), half)

    def swap(t):
        return pltpu.make_async_remote_copy(
            src_ref=give.at[t], dst_ref=take.at[t], send_sem=x_send.at[t], recv_sem=x_recv.at[t],
            device_id=(me, other), device_id_type=MESH,
        )

    def project(t, place):
        columns = pl.ds(pl.multiple_of(t * tile, tile), tile)
        a = jnp.concatenate([attn[j, place, :] for j in range(SIDE)], axis=1)
        return jnp.dot(a, w_ref[:, columns], preferred_element_type=jnp.float32)

    def from_peers(t, ds):
        columns = pl.ds(pl.multiple_of(t * tile, tile), tile)
        parts = [
            jnp.dot(attn[peer(d), theirs, :], w_ref[lanes(peer(d), width), columns], preferred_element_type=jnp.float32)
            for d in ds
        ]
        return functools.reduce(jnp.add, parts)

    def early_share(t, _):
        early[t] = from_peers(t, range(SIDE - 1))
        return 0

    lax.fori_loop(0, EARLY, early_share, 0)
    heads_in(SIDE - 1)

    def late_share(t, _):
        give[t] = (early[t] + from_peers(t, (SIDE - 1,))).astype(jnp.bfloat16)
        swap(t).start()
        return 0

    lax.fori_loop(0, EARLY, late_share, 0)

    def share(t, _):
        give[t] = project(t, theirs).astype(jnp.bfloat16)
        swap(t).start()
        return 0

    lax.fori_loop(EARLY, tiles, share, 0)

    def put(t):
        columns = pl.ds(pl.multiple_of(t * tile, tile), tile)
        return pltpu.make_async_copy(out_buf.at[:, columns], out_ref.at[:, columns], out_sem.at[t])

    def add_up(t, _):
        columns = pl.ds(pl.multiple_of(t * tile, tile), tile)
        swap(t).wait_recv()
        out_buf[:, columns] = (project(t, mine) + take[t].astype(jnp.float32)).astype(out_ref.dtype)
        put(t).start()
        return 0

    lax.fori_loop(0, tiles, add_up, 0)

    def swapped(t, _):
        swap(t).wait_send()
        return 0

    lax.fori_loop(0, tiles, swapped, 0)
    for d in range(1, SIDE):
        for part in range(2):
            pack_copy(part, d).wait_send()
        for copy in kv_copies(d):
            copy.wait_send()
        q_copy(d).wait_send()
        for pair in range(PAIRS):
            o_copies(peer(d), pair).wait_send()
    for copy in next_copies():
        copy.wait_send()
    for part in range(2):
        every = slots[part].at[pl.ds(0, (SIDE ** 3 - SIDE) * CAP)]
        remote(every, every, ring_send.at[part], slot_recv.at[part, 0], next_plane).wait_send()

    def stored(t, _):
        put(t).wait()
        return 0

    lax.fori_loop(0, tiles, stored, 0)


def on_device(n, queries, keys, values, vertical, slash, out_weight):
    rows = queries.shape[0]
    kv = vertical.shape[0]
    per_group = queries.shape[1] // (kv * HEAD_DIM)
    width = per_group * HEAD_DIM
    model = out_weight.shape[1]
    listed = vertical.shape[1]

    tile = math.gcd(model, 1024)
    tiles = model // tile
    dma = pltpu.SemaphoreType.DMA
    return pl.pallas_call(
        functools.partial(kernel, per_group, tile),
        out_shape=jax.ShapeDtypeStruct((rows // 2, model), jnp.bfloat16),
        in_specs=[pl.BlockSpec(memory_space=pl.ANY)] * 6,
        out_specs=pl.BlockSpec(memory_space=pl.ANY),
        scratch_shapes=[
            pltpu.VMEM(queries.shape, jnp.bfloat16),
            pltpu.VMEM(keys.shape, jnp.bfloat16),
            pltpu.VMEM(values.shape, jnp.bfloat16),
            pltpu.VMEM(vertical.shape, jnp.int32),
            pltpu.SMEM(vertical.shape, jnp.int32),
            pltpu.SMEM(slash.T.shape, jnp.int32),
            [pltpu.VMEM((kv, CAP, BLK, HEAD_DIM), jnp.bfloat16) for _ in range(2)],
            [pltpu.VMEM((n * CAP, BLK, HEAD_DIM), jnp.bfloat16) for _ in range(2)],
            pltpu.VMEM((SIDE, rows, width), jnp.bfloat16),
            pltpu.VMEM((SIDE, per_group, 2 * HEAD_DIM, rows), jnp.bfloat16),
            pltpu.VMEM((SIDE + 1, rows, HEAD_DIM), jnp.bfloat16),
            pltpu.VMEM((SIDE + 1, rows, HEAD_DIM), jnp.bfloat16),
            pltpu.VMEM((listed * BLK, HEAD_DIM), jnp.bfloat16),
            pltpu.SMEM((listed,), jnp.int32),
            pltpu.VMEM(out_weight.shape, jnp.bfloat16),
            pltpu.VMEM((SIDE, per_group, HEAD_DIM, rows), jnp.float32),
            pltpu.VMEM((SIDE, per_group, 1, rows), jnp.float32),
            pltpu.VMEM((SIDE, per_group, 1, rows), jnp.float32),
            pltpu.VMEM((SIDE, per_group, 1, rows), jnp.float32),
            pltpu.VMEM((SIDE, rows, width), jnp.bfloat16),
            pltpu.VMEM((SIDE, rows, width), jnp.bfloat16),
            pltpu.VMEM((EARLY, rows // 2, tile), jnp.float32),
            pltpu.VMEM((tiles, rows // 2, tile), jnp.bfloat16),
            pltpu.VMEM((tiles, rows // 2, tile), jnp.bfloat16),
            pltpu.VMEM((rows // 2, model), jnp.bfloat16),
            dma((6,)),
            dma,
            dma((2, SIDE)),
            dma((SIDE, 2)),
            dma((SIDE + 1, 2)),
            dma((SIDE,)),
            dma((SIDE,)),
            dma((2, ENDS + 1)),
            dma((2,)),
            dma((SIDE, PAIRS)),
            dma((SIDE, PAIRS)),
            dma((tiles,)),
            dma((tiles,)),
            dma((tiles,)),
        ],
        compiler_params=pltpu.CompilerParams(
            collective_id=0, has_side_effects=True, vmem_limit_bytes=60 * 2**20
        ),
    )(queries, keys, values, vertical, slash.T, out_weight)


def solution(mesh):
    placed = (
        P("seq", "head"),
        P("seq", "head"),
        P("seq", "head"),
        P("head", None),
        P("head", None),
        P("head", None),
    )
    return jax.shard_map(
        functools.partial(on_device, mesh.shape["seq"]),
        mesh=mesh, in_specs=placed, out_specs=P(("seq", "head"), None), check_vma=False,
    )
```

```python
import functools
import math

import jax
import jax.numpy as jnp
from jax import lax
from jax.experimental import pallas as pl
from jax.experimental.pallas import tpu as pltpu
from jax.sharding import PartitionSpec as P

HEAD_DIM = 128
BLK = 64
CAP = 2
NEGATIVE = -1e30
MESH = pl.DeviceIdType.MESH
SCALE = HEAD_DIM ** (-0.5) * math.log2(math.e)
SIDE = 4
FAR_CHUNK = 32
PAIRS = 2
FAR_PARTS = 2
ENDS = 2 * SIDE * SIDE
EARLY = 2
TOP_CHUNK = 32
AUX = 16


def kernel(
    per_group, tile,
    q_hbm, k_hbm, v_hbm, vert_hbm, slash_hbm, w_hbm, out_ref,
    q_ref, k_ref, v_ref, list_ref, vert_ref, slash_ref,
    packs, slots, qg, qt, kg, vg, aux_k, places, w_ref, acc, top, far_top, total, o_buf, attn, early, give, take, out_buf,
    in_sem, w_sem, pack_send, kv_send, kv_recv, q_send, q_recv, slot_recv, ring_send,
    o_send, o_recv, x_send, x_recv, out_sem,
):
    rows = q_ref.shape[0]
    me = lax.axis_index("seq")
    core = lax.axis_index("head")
    other = 1 - core
    o, c = me // SIDE, me % SIDE
    x, z = o // SIDE, o % SIDE
    slab_blocks = rows // BLK
    half = rows // 2
    width = per_group * HEAD_DIM
    chosen_count = vert_ref.shape[1]
    next_plane = (me + SIDE) % (SIDE ** 3)
    last_plane = (me + SIDE ** 3 - SIDE) % (SIDE ** 3)

    def at(xx, zz, cc):
        return (xx % SIDE * SIDE + zz % SIDE) * SIDE + cc

    given = [
        pltpu.make_async_copy(source, here, in_sem.at[i])
        for i, (source, here) in enumerate((
            (vert_hbm, list_ref), (k_hbm, k_ref), (v_hbm, v_ref), (q_hbm, q_ref), (vert_hbm, vert_ref),
            (slash_hbm, slash_ref)))
    ]
    for copy in given:
        copy.start()

    barrier = pltpu.get_barrier_semaphore()

    def greet(seq, head):
        pl.semaphore_signal(barrier, inc=1, device_id=(seq, head), device_id_type=MESH)

    greet(me, other)
    for d in range(1, SIDE):
        greet(o * SIDE + (c + d) % SIDE, core)
    for step in range(1, SIDE):
        greet(at(x + step, z, c), core)
        greet(at(x, z + step, c), core)
    greet(next_plane, core)
    greet(last_plane, core)

    weight_copy = pltpu.make_async_copy(w_hbm, w_ref, w_sem)
    weight_copy.start()

    def lanes(h, size=HEAD_DIM):
        return pl.ds(pl.multiple_of(h * size, size), size)

    first_block = me * slab_blocks
    for copy in given:
        copy.wait()
    found = list_ref[...] - first_block
    inside = (found >= 0) & (found < slab_blocks)
    low = jnp.min(jnp.where(inside, found, slab_blocks), axis=1, keepdims=True)
    high = jnp.max(jnp.where(inside, found, -1), axis=1, keepdims=True)
    for h in range(SIDE):
        for slot, extreme in enumerate((low, high)):
            pick = jnp.broadcast_to(extreme[h:h + 1], (BLK, HEAD_DIM))
            for part, source in enumerate((k_ref, v_ref)):
                got = source[:BLK, h * HEAD_DIM:(h + 1) * HEAD_DIM]
                for i in range(1, slab_blocks):
                    rows_i = source[i * BLK:(i + 1) * BLK, h * HEAD_DIM:(h + 1) * HEAD_DIM]
                    got = jnp.where(pick == i, rows_i, got)
                packs[part][h, slot] = got
    for part in range(2):
        for i in range(CAP):
            slots[part][me * CAP + i] = packs[part][c, i]
    kg[c + 1] = k_ref[:, lanes(c)]
    vg[c + 1] = v_ref[:, lanes(c)]
    qg[c] = q_ref[:, lanes(c, width)]

    pl.semaphore_wait(barrier, 1 + 3 * (SIDE - 1) + 2)

    def remote(src, dst, send_sem, recv_sem, seq):
        return pltpu.make_async_remote_copy(
            src_ref=src, dst_ref=dst, send_sem=send_sem, recv_sem=recv_sem,
            device_id=(seq, core), device_id_type=MESH,
        )

    def held(part, slab):
        return slots[part].at[pl.ds(slab * CAP, CAP)]

    def peer(d):
        return (c + d) % SIDE

    def pack_copy(part, d):
        return remote(packs[part].at[peer(d)], held(part, me), pack_send.at[part, d], slot_recv.at[part, c],
                      o * SIDE + peer(d))

    def kv_copies(d):
        to = peer(d)
        return [
            remote(source.at[:, lanes(to)], got.at[c + 1], kv_send.at[d, i], kv_recv.at[c + 1, i], o * SIDE + to)
            for i, (source, got) in enumerate(((k_ref, kg), (v_ref, vg)))
        ]

    def q_copy(d):
        to = peer(d)
        return remote(q_ref.at[:, lanes(to, width)], qg.at[c], q_send.at[d], q_recv.at[c], o * SIDE + to)

    def next_copies():
        return [
            remote(got.at[SIDE], got.at[0], kv_send.at[0, i], kv_recv.at[0, i], next_plane)
            for i, got in enumerate((kg, vg))
        ]

    near_order = (1, SIDE - 1, 2)
    for d in near_order:
        pack_copy(0, d).start()

    def slab_of(dp, dq, kind):
        x_first = kind < 2
        return jnp.where(x_first, at(x + SIDE - dp, z + SIDE - dq, kind), at(x + SIDE - dq, z + SIDE - dp, kind))

    def ring(part, slab, kind, phase, sign, mark):
        x_first = kind < 2
        along_x = x_first if phase == 0 else jnp.logical_not(x_first)
        to = jnp.where(along_x, at(x + SIDE + sign, z, c), at(x, z + SIDE + sign, c))
        there = held(part, slab)
        return remote(there, there, ring_send.at[part], slot_recv.at[part, mark], to)

    def in_group(kind):
        return kind

    def in_first(dp, kind):
        return SIDE + (dp % SIDE - 1) * SIDE + kind

    def in_second(dp, sign, kind):
        return jnp.where(kind % 2 == (1 - sign) // 2, SIDE * (SIDE + dp % SIDE) + kind, ENDS)

    def arrived(part, slab, mark):
        there = held(part, slab)
        remote(there, there, pack_send.at[part, 1], slot_recv.at[part, mark], next_plane).wait_recv()

    def first(part, ds=(0, SIDE - 1, 1, 2)):
        for d in ds:
            kind = peer(d)
            for dp in (1, -1, 2):
                slab = slab_of(dp, 0, kind)
                arrived(part, slab, in_first(dp, kind))
                for sign in (1, -1):
                    ring(part, slab, kind, 1, sign, in_second(dp, sign, kind)).start()

    def second(part, dp):
        for kind in range(SIDE):
            sign = 1 if kind % 2 == 0 else -1
            slab = slab_of(dp, sign, kind)
            arrived(part, slab, in_second(dp, sign, kind))
            ring(part, slab, kind, 1, sign, ENDS).start()

    def pass_own(part, ds):
        for d in ds:
            slab = o * SIDE + peer(d)
            kind = peer(d)
            if d:
                arrived(part, slab, in_group(kind))
            for step in (1, -1, 2):
                ring(part, slab, kind, 0, step, in_first(step, kind)).start()
            for sign in (1, -1):
                ring(part, slab, kind, 1, sign, in_second(0, sign, kind)).start()

    pass_own(0, (0,))
    lane = lax.broadcasted_iota(jnp.int32, (BLK, HEAD_DIM), 1)
    limit = (o * SIDE + lane - 1) * slab_blocks
    unit = jnp.where((lane >= SIDE) & (lane < SIDE + 3), 1.0, 0.0)

    def look_up(n, _):
        for j in range(8):
            e = n * 8 + j
            block = vert_ref[c, e]
            slab = block // slab_blocks
            before = jnp.where(e > 0, vert_ref[c, jnp.maximum(e - 1, 0)] // slab_blocks, -1)
            places[e] = slab * CAP + jnp.where(before == slab, 1, 0)
            mask = jnp.where((lane < SIDE) & (block >= limit), NEGATIVE, unit)
            aux_k[pl.ds(pl.multiple_of(e * BLK, BLK), BLK), :] = mask.astype(jnp.bfloat16)
        return 0

    lax.fori_loop(0, chosen_count // 8, look_up, 0)
    pass_own(0, (SIDE - 1, 1, 2))
    for d in near_order:
        for copy in kv_copies(d):
            copy.start()
    for d in near_order:
        pack_copy(1, d).start()
    for d in (SIDE - 1, 1, 2):
        q_copy(d).start()
    first(0)

    heads = range(per_group)

    def turn(i):
        row = lax.broadcasted_iota(jnp.int32, (HEAD_DIM, rows), 0)
        for g in heads:
            qt[i, g, :HEAD_DIM] = qg[i, :, g * HEAD_DIM:(g + 1) * HEAD_DIM].T
            qt[i, g, HEAD_DIM:] = jnp.where(row == i, 1.0, 0.0).astype(jnp.bfloat16)

    def near(i):
        base = (o * SIDE + i) * slab_blocks
        k = jnp.concatenate([kg[i], kg[i + 1]], axis=0)
        vt = jnp.concatenate([vg[i], vg[i + 1]], axis=0).T
        shape = (2 * slab_blocks, rows)
        block = lax.broadcasted_iota(jnp.int32, shape, 0) - slab_blocks
        gap = lax.broadcasted_iota(jnp.int32, shape, 1) // BLK - block
        block = base + block
        good = gap == 0
        for j in range(slash_ref.shape[0]):
            good = good | (gap == slash_ref[j, c])
        chosen = block == vert_ref[c, 0]
        for e in range(1, chosen_count):
            chosen = chosen | (block == vert_ref[c, e])
        good = good | (chosen & (gap > 0))
        bias = jnp.where(good & (block >= 0), 0.0, NEGATIVE)
        keys_at = lax.broadcasted_iota(jnp.int32, (rows, rows), 0)
        query_at = lax.broadcasted_iota(jnp.int32, (rows, rows), 1)
        causal = keys_at <= query_at
        scores = []
        for g in heads:
            scores.append(jnp.dot(k, qt[i, g, :HEAD_DIM], preferred_element_type=jnp.float32))
        for g, s in zip(heads, scores):
            s = jnp.concatenate(
                [s[j * BLK:(j + 1) * BLK] + bias[j:j + 1] for j in range(2 * slab_blocks)], axis=0)
            s = jnp.concatenate([s[:rows], jnp.where(causal, s[rows:], NEGATIVE)], axis=0)
            peak = jnp.max(s, axis=0, keepdims=True)
            p = jnp.exp2((s - peak) * SCALE)
            top[i, g] = peak
            total[i, g] = jnp.sum(p, axis=0, keepdims=True)
            acc[i, g] = jnp.dot(vt, p.astype(jnp.bfloat16), preferred_element_type=jnp.float32)

    def second_keys(dp, _):
        second(0, dp)
        return 0

    def last_ones(part):
        every = slots[part].at[pl.ds(0, 2 * SIDE * SIDE * CAP)]
        remote(every, every, pack_send.at[part, 1], slot_recv.at[part, ENDS], next_plane).wait_recv()

    lax.fori_loop(0, SIDE, second_keys, 0)
    pass_own(1, (0, SIDE - 1, 1, 2))
    for d in range(1, SIDE):
        for i, got in enumerate((kg, vg)):
            there = got.at[peer(d) + 1]
            remote(there, there, kv_send.at[d, i], kv_recv.at[peer(d) + 1, i], next_plane).wait_recv()
    for copy in next_copies():
        copy.start()

    def queries_in(i):
        remote(qg.at[i], qg.at[i], q_send.at[1], q_recv.at[i], next_plane).wait_recv()

    turn(c)

    @pl.when(c > 0)
    def _():
        near(c)

    last_ones(0)

    def blocks(part, n, size):
        return jnp.concatenate([slots[part][places[n * size + j]] for j in range(size)], axis=0)

    def keys_of(n, size):
        masks = aux_k[pl.ds(pl.multiple_of(n * size * BLK, size * BLK), size * BLK), :]
        return jnp.concatenate([blocks(0, n, size), masks], axis=1)

    def steps(size):
        return jnp.minimum(chosen_count, (o * SIDE + 2) * CAP + size - 1) // size

    def largest(i):
        def chunk(n, peaks):
            k = keys_of(n, TOP_CHUNK)
            return tuple(
                jnp.maximum(peak, jnp.max(jnp.dot(k, qt[i, g], preferred_element_type=jnp.float32),
                                          axis=0, keepdims=True))
                for g, peak in zip(heads, peaks))

        peaks = lax.fori_loop(0, steps(TOP_CHUNK), chunk, (jnp.full((1, rows), NEGATIVE),) * per_group)
        for g, peak in zip(heads, peaks):
            far_top[i, g] = peak

    def join(i):
        row = lax.broadcasted_iota(jnp.int32, (AUX, rows), 0)
        for g in heads:
            old = top[i, g]
            peak = jnp.maximum(old, far_top[i, g])
            shrink = jnp.exp2((old - peak) * SCALE)
            total[i, g] = total[i, g] * shrink
            acc[i, g] = acc[i, g] * shrink
            rest = -peak
            aux = jnp.where(row == i, 1.0, 0.0)
            for j in range(3):
                part = rest.astype(jnp.bfloat16).astype(jnp.float32)
                aux = jnp.where(row == SIDE + j, part, aux)
                rest = rest - part
            qt[i, g, HEAD_DIM:HEAD_DIM + AUX] = aux.astype(jnp.bfloat16)

    def first_pass(step, _):
        i = (c + step + jnp.where(step == 2, 1, jnp.where(step == 3, -1, 0))) % SIDE

        @pl.when(step > 0)
        def _():
            queries_in(i)
            turn(i)

        largest(i)

        @pl.when(step == 0)
        def _():
            first(1, (0, SIDE - 1))

        @pl.when(step == 1)
        def _():
            first(1, (1, 2))

        def values_second(j, _):
            second(1, (2 + j) % SIDE)
            return 0

        lax.fori_loop(jnp.where(step == 2, 0, SIDE), SIDE, values_second, 0)
        return 0

    lax.fori_loop(0, SIDE, first_pass, 0)
    for copy in next_copies():
        copy.wait_recv()

    def other_near(i, _):
        @pl.when(i != c)
        def _():
            near(i)

        return 0

    lax.fori_loop(0, SIDE, other_near, 0)
    last_ones(1)

    def o_copies(i, pair):
        columns = pl.ds(pair * width // PAIRS, width // PAIRS)
        return remote(o_buf.at[i, :, columns], attn.at[c, :, columns], o_send.at[i, pair], o_recv.at[c, pair], o * SIDE + i)

    def far_slab(step, _):
        i = (c + SIDE - 1 - step) % SIDE

        @pl.when((step == SIDE - 1) & (c == 0))
        def _():
            near(i)

        join(i)
        for pair in range(PAIRS):
            some = heads[pair * per_group // PAIRS:(pair + 1) * per_group // PAIRS]

            def part_of_list(n):
                k = keys_of(n, FAR_CHUNK)
                v = blocks(1, n, FAR_CHUNK)
                scores = [jnp.dot(k, qt[i, g], preferred_element_type=jnp.float32) for g in some]
                old = [(total[i, g], acc[i, g]) for g in some]
                new = []
                for s, (amount, mix) in zip(scores, old):
                    p = jnp.exp2(s * SCALE)
                    amount = amount + jnp.sum(p, axis=0, keepdims=True)
                    mix = mix + lax.dot_general(v, p.astype(jnp.bfloat16), (((0,), (0,)), ((), ())),
                                                preferred_element_type=jnp.float32)
                    new.append((amount, mix))
                for g, (amount, mix) in zip(some, new):
                    total[i, g] = amount
                    acc[i, g] = mix

            def chunk(n, _):
                for j in range(FAR_PARTS):
                    part_of_list(n * FAR_PARTS + j)
                return 0

            lax.fori_loop(0, steps(FAR_CHUNK * FAR_PARTS), chunk, 0)
            for g in some:
                a = acc[i, g] * (1.0 / total[i, g])
                o_buf[i, :, g * HEAD_DIM:(g + 1) * HEAD_DIM] = a.T.astype(jnp.bfloat16)

            @pl.when(step < SIDE - 1)
            def _():
                o_copies(i, pair).start()

        return 0

    lax.fori_loop(0, SIDE, far_slab, 0)
    attn[c] = o_buf[c]

    def heads_in(d):
        for pair in range(PAIRS):
            there = attn.at[peer(d), :, pl.ds(pair * width // PAIRS, width // PAIRS)]
            remote(there, there, o_send.at[peer(d), pair], o_recv.at[peer(d), pair], next_plane).wait_recv()

    for d in range(1, SIDE - 1):
        heads_in(d)

    weight_copy.wait()
    tiles = give.shape[0]
    mine = pl.ds(pl.multiple_of(core * half, half), half)
    theirs = pl.ds(pl.multiple_of(other * half, half), half)

    def swap(t):
        return pltpu.make_async_remote_copy(
            src_ref=give.at[t], dst_ref=take.at[t], send_sem=x_send.at[t], recv_sem=x_recv.at[t],
            device_id=(me, other), device_id_type=MESH,
        )

    def project(t, place):
        columns = pl.ds(pl.multiple_of(t * tile, tile), tile)
        a = jnp.concatenate([attn[j, place, :] for j in range(SIDE)], axis=1)
        return jnp.dot(a, w_ref[:, columns], preferred_element_type=jnp.float32)

    def from_peers(t, ds):
        columns = pl.ds(pl.multiple_of(t * tile, tile), tile)
        parts = [
            jnp.dot(attn[peer(d), theirs, :], w_ref[lanes(peer(d), width), columns], preferred_element_type=jnp.float32)
            for d in ds
        ]
        return functools.reduce(jnp.add, parts)

    def early_share(t, _):
        early[t] = from_peers(t, range(SIDE - 1))
        return 0

    lax.fori_loop(0, EARLY, early_share, 0)
    heads_in(SIDE - 1)

    def late_share(t, _):
        give[t] = (early[t] + from_peers(t, (SIDE - 1,))).astype(jnp.bfloat16)
        swap(t).start()
        return 0

    lax.fori_loop(0, EARLY, late_share, 0)

    def share(t, _):
        give[t] = project(t, theirs).astype(jnp.bfloat16)
        swap(t).start()
        return 0

    lax.fori_loop(EARLY, tiles, share, 0)

    def put(t):
        columns = pl.ds(pl.multiple_of(t * tile, tile), tile)
        return pltpu.make_async_copy(out_buf.at[:, columns], out_ref.at[:, columns], out_sem.at[t])

    def add_up(t, _):
        columns = pl.ds(pl.multiple_of(t * tile, tile), tile)
        swap(t).wait_recv()
        out_buf[:, columns] = (project(t, mine) + take[t].astype(jnp.float32)).astype(out_ref.dtype)
        put(t).start()
        return 0

    lax.fori_loop(0, tiles, add_up, 0)

    def swapped(t, _):
        swap(t).wait_send()
        return 0

    lax.fori_loop(0, tiles, swapped, 0)
    for d in range(1, SIDE):
        for part in range(2):
            pack_copy(part, d).wait_send()
        for copy in kv_copies(d):
            copy.wait_send()
        q_copy(d).wait_send()
        for pair in range(PAIRS):
            o_copies(peer(d), pair).wait_send()
    for copy in next_copies():
        copy.wait_send()
    for part in range(2):
        every = slots[part].at[pl.ds(0, (SIDE ** 3 - SIDE) * CAP)]
        remote(every, every, ring_send.at[part], slot_recv.at[part, 0], next_plane).wait_send()

    def stored(t, _):
        put(t).wait()
        return 0

    lax.fori_loop(0, tiles, stored, 0)


def on_device(n, queries, keys, values, vertical, slash, out_weight):
    rows = queries.shape[0]
    kv = vertical.shape[0]
    per_group = queries.shape[1] // (kv * HEAD_DIM)
    width = per_group * HEAD_DIM
    model = out_weight.shape[1]
    listed = vertical.shape[1]

    tile = math.gcd(model, 1024)
    tiles = model // tile
    dma = pltpu.SemaphoreType.DMA
    return pl.pallas_call(
        functools.partial(kernel, per_group, tile),
        out_shape=jax.ShapeDtypeStruct((rows // 2, model), jnp.bfloat16),
        in_specs=[pl.BlockSpec(memory_space=pl.ANY)] * 6,
        out_specs=pl.BlockSpec(memory_space=pl.ANY),
        scratch_shapes=[
            pltpu.VMEM(queries.shape, jnp.bfloat16),
            pltpu.VMEM(keys.shape, jnp.bfloat16),
            pltpu.VMEM(values.shape, jnp.bfloat16),
            pltpu.VMEM(vertical.shape, jnp.int32),
            pltpu.SMEM(vertical.shape, jnp.int32),
            pltpu.SMEM(slash.T.shape, jnp.int32),
            [pltpu.VMEM((kv, CAP, BLK, HEAD_DIM), jnp.bfloat16) for _ in range(2)],
            [pltpu.VMEM((n * CAP, BLK, HEAD_DIM), jnp.bfloat16) for _ in range(2)],
            pltpu.VMEM((SIDE, rows, width), jnp.bfloat16),
            pltpu.VMEM((SIDE, per_group, 2 * HEAD_DIM, rows), jnp.bfloat16),
            pltpu.VMEM((SIDE + 1, rows, HEAD_DIM), jnp.bfloat16),
            pltpu.VMEM((SIDE + 1, rows, HEAD_DIM), jnp.bfloat16),
            pltpu.VMEM((listed * BLK, HEAD_DIM), jnp.bfloat16),
            pltpu.SMEM((listed,), jnp.int32),
            pltpu.VMEM(out_weight.shape, jnp.bfloat16),
            pltpu.VMEM((SIDE, per_group, HEAD_DIM, rows), jnp.float32),
            pltpu.VMEM((SIDE, per_group, 1, rows), jnp.float32),
            pltpu.VMEM((SIDE, per_group, 1, rows), jnp.float32),
            pltpu.VMEM((SIDE, per_group, 1, rows), jnp.float32),
            pltpu.VMEM((SIDE, rows, width), jnp.bfloat16),
            pltpu.VMEM((SIDE, rows, width), jnp.bfloat16),
            pltpu.VMEM((EARLY, rows // 2, tile), jnp.float32),
            pltpu.VMEM((tiles, rows // 2, tile), jnp.bfloat16),
            pltpu.VMEM((tiles, rows // 2, tile), jnp.bfloat16),
            pltpu.VMEM((rows // 2, model), jnp.bfloat16),
            dma((6,)),
            dma,
            dma((2, SIDE)),
            dma((SIDE, 2)),
            dma((SIDE + 1, 2)),
            dma((SIDE,)),
            dma((SIDE,)),
            dma((2, ENDS + 1)),
            dma((2,)),
            dma((SIDE, PAIRS)),
            dma((SIDE, PAIRS)),
            dma((tiles,)),
            dma((tiles,)),
            dma((tiles,)),
        ],
        compiler_params=pltpu.CompilerParams(
            collective_id=0, has_side_effects=True, vmem_limit_bytes=60 * 2**20
        ),
    )(queries, keys, values, vertical, slash.T, out_weight)


def solution(mesh):
    placed = (
        P("seq", "head"),
        P("seq", "head"),
        P("seq", "head"),
        P("head", None),
        P("head", None),
        P("head", None),
    )
    return jax.shard_map(
        functools.partial(on_device, mesh.shape["seq"]),
        mesh=mesh, in_specs=placed, out_specs=P(("seq", "head"), None), check_vma=False,
    )
```
